128 devices in a mesh: ctx: 16 (over z, y), dp: 8 (over x, core).
Axes of the slice: x: 4, y: 4, z: 4, core: 2. Of those that a mesh axis runs over, the one named last changes fastest.
Arguments:
- grad_out: bfloat16 [8, 6144, 4096], P('dp', 'ctx'), may hold values from -6 to 6
- hidden: bfloat16 [8, 6144, 1792], P('dp', 'ctx'), may hold values from -6 to 6
- down_weight: bfloat16 [1792, 4096], replicated, may hold values from -0.09375 to 0.09375
Outputs:
- grad_hidden: bfloat16 [8, 6144, 1792], P('dp', 'ctx')
- weight_grad: float32 [1792, 4096], P('ctx', 'dp')
- hidden_amax: float32 [8, 1792], P('dp', 'ctx')
- grad_amax: float32 [8, 4096], P('dp', 'ctx')
The draws below stay inside these ranges and needn't reach their ends.
All inputs are finite; a program needn't handle non-finite values.
Results may differ from the reference program's by a relative error of at most 0.006.
Values may be sent and summed in bfloat16 or wider, within the bound.
A program may use at most 192 MiB of HBM per device.

```python
import jax
import jax.numpy as jnp
from jax import lax

D = 4096
FFS = 1792
SEQ = 6144
REPLICAS = 8


def level_of(own_key, dims, pieces, low, top_value):
    level, own = 1.0, jax.random.fold_in(own_key, 6)
    for dim, shards_of in pieces:
        heights = jnp.exp(jax.random.uniform(jax.random.fold_in(own, dim), (shards_of,), jnp.float32, low / len(pieces), top_value / len(pieces)))
        level = level * jnp.repeat(heights, dims[dim] // shards_of).reshape([-1 if axis == dim else 1 for axis in range(len(dims))])
    return level


def noise(stream_key, extent, spread, reach, split=(), dtype=jnp.bfloat16):
    array = spread * jax.random.normal(stream_key, extent, jnp.float32)
    if split:
        array = array * level_of(stream_key, extent, split, -0.22, 0.18)
    return jnp.clip(array, -reach, reach).astype(dtype)


def setup_inputs(seed: int = 0) -> dict:
    key_list = jax.random.split(jax.random.key(seed), 4)
    grad_out = noise(key_list[0], (REPLICAS, SEQ, D), 1.0, 6.0, ((0, 8), (1, 16)))
    hidden = noise(key_list[1], (REPLICAS, SEQ, FFS), 1.0, 6.0, ((0, 8), (1, 16)))
    down_weight = noise(key_list[2], (FFS, D), D ** -0.5, 0.09375)
    return dict(grad_out=grad_out, hidden=hidden, down_weight=down_weight)


ceiling = 448.0

def to_grid(values, peaks):
    scaled = values.astype(jnp.float32) * (ceiling / peaks)[None, :]
    magnitude = jnp.abs(scaled)
    spacing = jnp.full_like(magnitude, 2.0 ** (-9))
    for exponent in range(-5, 9):
        spacing = jnp.where(magnitude >= 2.0 ** exponent, 2.0 ** (exponent - 3), spacing)
    snapped = jnp.floor(magnitude / spacing + 0.5) * spacing
    return jnp.where(scaled < 0, -snapped, snapped).astype(jnp.bfloat16)

def reference(grad_out, hidden, down_weight):
    hidden_amax = jnp.maximum(lax.optimization_barrier(jnp.max(jnp.abs(hidden.astype(jnp.float32)), axis=1)), 1.0)
    grad_amax = jnp.maximum(lax.optimization_barrier(jnp.max(jnp.abs(grad_out.astype(jnp.float32)), axis=1)), 1.0)
    total = jnp.zeros((FFS, D), jnp.float32)
    results = []
    for replica in range(REPLICAS):
        gdata = grad_out[replica]
        hdata = hidden[replica]
        results.append(lax.dot_general(gdata, down_weight, (((1,), (1,)), ((), ())), preferred_element_type=jnp.float32).astype(jnp.bfloat16))
        hquant = to_grid(hdata, hidden_amax[replica])
        gquant = to_grid(gdata, grad_amax[replica])
        product = lax.dot_general(hquant, gquant, (((0,), (0,)), ((), ())), preferred_element_type=jnp.float32)
        total = total + product * (hidden_amax[replica] / ceiling)[:, None] * (grad_amax[replica] / ceiling)[None, :]
    weight_grad = total / jnp.sqrt(jnp.float32(SEQ * REPLICAS))
    grad_hidden = jnp.stack(results, axis=0)
    return (grad_hidden, weight_grad, hidden_amax, grad_amax)
```

```python
import functools

import jax
import jax.numpy as jnp
import numpy as np
from jax import lax
from jax.experimental import pallas as pl
from jax.experimental.pallas import tpu as pltpu
from jax.sharding import PartitionSpec as P

CEILING = 448.0
D, FFS, SEQ, REPLICAS = 4096, 1792, 6144, 8
TOK = 384
F8 = jnp.float8_e4m3fn
BF = jnp.bfloat16
F32 = jnp.float32
MESH = pl.DeviceIdType.MESH
NUDGE = np.float32((1 + 2.0**-21) * 2.0**-10)
ROWS = 112
EXTRA = ((0, 32), (32, 32), (64, 48))
PEAKS = FFS + D
GH = 256
SPLIT = 80


def kernel(g_hbm, h_hbm, w_hbm, gh_hbm, wg_ref, pk_out,
           g_own, h_own, g_peer, h_peer, w_v, gh_v, hqt, gq, hdc, gsr, acc, acce, pk,
           stage, am1, am2, am3, amy, amz, amp,
           own0, own1, own2, r10, r11, r12, r20, r21, r22, r30, r31, r32,
           lsem, wsem, osem, ssem, rsem, s2, q2):
    ctx = lax.axis_index("ctx")
    dp = lax.axis_index("dp")
    z, y, x, c = ctx // 4, ctx % 4, dp // 2, dp % 2
    own, rx1, rx2, rx3 = (own0, own1, own2), (r10, r11, r12), (r20, r21, r22), (r30, r31, r32)
    heights = (144, 144, 160)

    def dev(axis, step):
        zz, yy, xx, cc = z, y, x, c
        if axis == "z":
            zz = (z + step) % 4
        elif axis == "y":
            yy = (y + step) % 4
        elif axis == "x":
            xx = (x + step) % 4
        else:
            cc = 1 - c
        return (zz * 4 + yy, xx * 2 + cc)

    lh = pltpu.make_async_copy(h_hbm, h_own, lsem.at[0])
    lh.start()
    lg = []
    for i in range(4):
        at = pl.ds(i * 1024, 1024)
        lg.append(pltpu.make_async_copy(g_hbm.at[:, at], g_own.at[:, at], lsem.at[1 + i]))
        lg[-1].start()

    def wcopy(j):
        at = pl.ds(pl.multiple_of(j * GH, GH), GH)
        return pltpu.make_async_copy(w_hbm.at[at, :], w_v.at[at, :], wsem.at[j])

    for j in range(FFS // GH):
        wcopy(j).start()

    barrier = pltpu.get_barrier_semaphore()
    friends = [dev("y", d) for d in (1, 2, 3)] + [dev("z", d) for d in (1, 2, 3)]
    friends += [dev("x", 1), dev("x", 3), dev("c", 1)]
    for f in friends:
        pl.semaphore_signal(barrier, inc=1, device_id=f, device_id_type=MESH)

    sends = []

    def remote(src, dst, i, to, sems=None):
        a, b = sems or (ssem, rsem)
        copy = pltpu.make_async_remote_copy(
            src_ref=src, dst_ref=dst, send_sem=a.at[i], recv_sem=b.at[i],
            device_id=to, device_id_type=MESH)
        copy.start()
        sends.append(copy)
        return copy

    small = (s2, q2)

    def peak_row(ref, lo, size):
        at = pl.ds(pl.multiple_of(lo, 128), size)
        return jnp.max(jnp.abs(ref[:, at].astype(F32)), axis=0, keepdims=True)

    stage[...] = jnp.zeros_like(stage)
    lh.wait()

    def h_peaks(i, _):
        at = pl.multiple_of(i * 256, 256)
        pk[0, :, pl.ds(at, 256)] = peak_row(h_own, at, 256)
        return 0

    lax.fori_loop(0, FFS // 256, h_peaks, 0)
    pl.semaphore_wait(barrier, len(friends))
    peer = dev("c", 1)
    swaps = [remote(h_own, h_peer, 0, peer, small)]
    for i in range(4):
        lg[i].wait()
        src = pl.ds(pl.multiple_of(i * 1024 + (1 - c) * 512, 512), 512)
        swaps.append(remote(g_own.at[:, src], g_peer.at[:, pl.ds(i * 512, 512)], 1 + i, peer, small))

        def g_peaks(k, _, i=i):
            at = pl.multiple_of(i * 1024 + k * 256, 256)
            pk[0, :, pl.ds(FFS + at, 256)] = peak_row(g_own, at, 256)
            return 0

        lax.fori_loop(0, 4, g_peaks, 0)

    def spread(n):
        for r in range(16):
            size = 384 if r < 15 else 128
            yield r, slice(0, size), slice(r * 384, r * 384 + size)

    for r, a, b in spread(16):
        stage[r : r + 1, a] = pk[0, :, b]
    am1[...] = stage[...].astype(BF)
    gets = [remote(am1, amy.at[d - 1], 5 + d - 1, dev("y", d), small) for d in (1, 2, 3)]

    def gh_step(j, _):
        wcopy(j).wait()
        at = pl.ds(pl.multiple_of(j * GH, GH), GH)
        res = lax.dot_general(
            g_own[...], w_v[at, :], (((1,), (1,)), ((), ())), preferred_element_type=F32)
        gh_v[:, at] = res.astype(BF)
        return 0

    lax.fori_loop(0, 2, gh_step, 0)
    for e in gets:
        e.wait_recv()
    am2[...] = jnp.maximum(
        jnp.maximum(am1[...].astype(F32), amy[0].astype(F32)),
        jnp.maximum(amy[1].astype(F32), amy[2].astype(F32))).astype(BF)
    gets = [remote(am2, amz.at[d - 1], 8 + d - 1, dev("z", d), small) for d in (1, 2, 3)]
    lax.fori_loop(2, 4, gh_step, 0)
    for e in gets:
        e.wait_recv()
    top = jnp.maximum(
        jnp.maximum(am2[...].astype(F32), amz[0].astype(F32)),
        jnp.maximum(amz[1].astype(F32), amz[2].astype(F32)))
    am3[...] = top.astype(BF)
    swap_peaks = remote(am3, amp, 11, peer, small)

    def unpack(r, values):
        stage[...] = jnp.maximum(values, 1.0)
        for k, a, b in spread(16):
            pk[r, :, b] = stage[k : k + 1, a]

    unpack(0, top)
    pk_out[...] = pk[0]

    def on_grid(values, peaks):
        v = values.astype(F32) * ((CEILING / peaks) * 1024.0)
        return (v.astype(jnp.int32).astype(F32) * NUDGE).astype(F8)

    def quantize(r, href, gref, wide, offset):
        def h_step(i, _):
            at = pl.ds(pl.multiple_of(i * 256, 256), 256)
            peaks = pk[r, :, at]
            hqt[r, at, :] = on_grid(href[:, at], peaks).astype(BF).T
            tall = jnp.broadcast_to(peaks / CEILING, (128, 256)).T
            hdc[r, at, :] = tall
            return 0

        lax.fori_loop(0, FFS // 256, h_step, 0)

        def g_step(i, _):
            q, xr = i // 4, i % 4
            xx = (x + xr) % 4
            at = pl.ds(pl.multiple_of(xx * wide + offset + q * 128, 128), 128)
            pat = pl.ds(pl.multiple_of(FFS + xx * 1024 + c * 512 + q * 128, 128), 128)
            to = pl.ds(pl.multiple_of(xr * 128, 128), 128)
            peaks = pk[r, :, pat]
            gq[r, q, :, to] = on_grid(gref[:, at], peaks).astype(BF)
            gsr[r, q, :, to] = peaks / CEILING
            return 0

        lax.fori_loop(0, 16, g_step, 0)

    quantize(0, h_own, g_own, 1024, c * 512)
    swap_peaks.wait_recv()
    unpack(1, amp[...].astype(F32))
    for e in swaps:
        e.wait_recv()
    quantize(1, h_peer, g_peer, 512, 0)

    def gather(ref, r, offsets, size):
        return jnp.concatenate(
            [ref[r, pl.ds(pl.multiple_of(o, 16), size), :] for o in offsets], axis=0)

    def product(q, offsets, size, total):
        for r in range(2):
            left = gather(hqt, r, offsets, size)
            res = jnp.dot(left, gq[r, q], preferred_element_type=F32)
            tall = gather(hdc, r, offsets, size)
            res = res * jnp.concatenate([tall] * 4, axis=1) * gsr[r, q]
            if r == 0:
                total[...] = res
            else:
                return (res + total[...]).astype(BF)

    def task(p, k):
        if p == 1:
            base = [o * 448 + ((y + k) % 4) * ROWS for o in range(4)]
        else:
            base = [((z + k) % 4) * 448 + o * ROWS for o in range(4)]
        lo, size = EXTRA[p]
        main = product(p, base, ROWS, acc)
        more = product(3, [b + lo for b in base], size, acce.at[pl.ds(0, 4 * size)])
        for o in range(4):
            away = (o - z) % 4 if p == 1 else (o - y) % 4
            for xr in range(4):
                if p == 0:
                    to = own0.at[k, away, xr]
                elif p == 1:
                    to = own1.at[k, xr, away]
                else:
                    to = own2.at[xr, k, away]
                cols = slice(xr * 128, xr * 128 + 128)
                to[0:ROWS, :] = main[o * ROWS : (o + 1) * ROWS, cols]
                to[ROWS : ROWS + size, :] = more[o * size : (o + 1) * size, cols]

    axes = (("z", "y", "x"), ("y", "x", "z"), ("x", "z", "y"))

    def piece(ph, p, k, half):
        if ph == 0:
            return own[p].at[k, pl.ds(2 * half, 2)]
        if ph == 1:
            return own[p].at[0, k, pl.ds(2 * half, 2)]
        rows = pl.ds(0, SPLIT) if half == 0 else pl.ds(SPLIT, heights[p] - SPLIT)
        return own[p].at[0, 0, k, rows]

    def landing(ph, p, m, half):
        ref = (rx1, rx2, rx3)[ph][p].at[m]
        if ph == 2:
            return ref.at[pl.ds(0, SPLIT if half == 0 else heights[p] - SPLIT)]
        return ref

    flights = {}
    plan = {
        "a+": (0, 0, 2, 0), "c+": (0, 1, 1, 1), "b+": (0, 2, 1, 0),
        "a-": (1, 3, 2, 1), "c-": (1, 4, 3, 0), "b-": (1, 5, 3, 1),
    }

    def post(ph, p, name):
        way, m, k, half = plan[name]
        to = dev(axes[p][ph], 1 if way == 0 else 3)
        flights[ph, p, name] = remote(
            piece(ph, p, k, half), landing(ph, p, m, half), (ph * 3 + p) * 6 + m, to)

    def arrived(ph, p, name):
        flights[ph, p, name].wait_recv()
        _, m, _, half = plan[name]
        return landing(ph, p, m, half)

    def add_into(ref, others):
        total = ref[...].astype(F32)
        for o in others:
            total = total + o[...].astype(F32)
        ref[...] = total.astype(BF)

    def onward(ph, p):
        for sign, k, half in (("+", 1, 0), ("-", 3, 1)):
            got = arrived(ph, p, "a" + sign)
            mine = piece(ph, p, k, half)
            if ph == 0:
                def step(i, _, mine=mine, got=got):
                    add_into(mine.at[i // 4, i % 4], [got.at[i // 4, i % 4]])
                    return 0
                lax.fori_loop(0, 8, step, 0)
            elif ph == 1:
                for i in range(2):
                    add_into(mine.at[i], [got.at[i]])
            else:
                add_into(mine, [got])
            post(ph, p, "b" + sign)

    def gather_all(ph, p):
        refs = {n: arrived(ph, p, n) for n in ("c+", "c-", "b+", "b-")}
        return (refs["b+"], refs["c-"]), (refs["c+"], refs["b-"])

    task(0, 2)
    post(0, 0, "a+"), post(0, 0, "a-")
    task(1, 2)
    post(0, 1, "a+"), post(0, 1, "a-")

    def x_task(k, _):
        task(2, k)
        return 0

    lax.fori_loop(0, 4, x_task, 0)
    for n in ("a+", "a-", "c+", "c-"):
        post(0, 2, n)
    for p in (0, 1):
        def rest(j, _, p=p):
            task(p, (1 + 2 * j) % 5)
            return 0

        lax.fori_loop(0, 3, rest, 0)
        post(0, p, "c+"), post(0, p, "c-")

    lax.fori_loop(4, FFS // GH, gh_step, 0)
    gh_copy = pltpu.make_async_copy(gh_v, gh_hbm, osem)
    gh_copy.start()

    for p in range(3):
        onward(0, p)
    for p in range(3):
        pair = gather_all(0, p)
        for k in (2, 1, 3, 0):
            def step(i, _, k=k, pair=pair, p=p):
                add_into(own[p].at[0, k, i], [o.at[k % 2, i] for o in pair[k // 2]])
                return 0

            lax.fori_loop(0, 4, step, 0)
            if k == 2:
                post(1, p, "a+"), post(1, p, "a-")
            elif k == 1:
                post(1, p, "c+")
            elif k == 3:
                post(1, p, "c-")
    for p in range(3):
        onward(1, p)
    for p in range(3):
        pair = gather_all(1, p)
        for k in (2, 1, 3, 0):
            add_into(own[p].at[0, 0, k], [o.at[k % 2] for o in pair[k // 2]])
            if k == 2:
                post(2, p, "a+"), post(2, p, "a-")
            elif k == 1:
                post(2, p, "c+")
            elif k == 3:
                post(2, p, "c-")
    for p in range(3):
        onward(2, p)
    for p in range(3):
        pair = gather_all(2, p)
        cols = slice(p * 128, p * 128 + 128)
        lo, size = EXTRA[p]
        for half in (0, 1):
            total = piece(2, p, 0, half)[...].astype(F32)
            for o in pair[half]:
                total = total + o[...].astype(F32)
            if half == 0:
                wg_ref[0:SPLIT, cols] = total
            else:
                wg_ref[SPLIT:ROWS, cols] = total[: ROWS - SPLIT]
                wg_ref[lo : lo + size, 384:512] = total[ROWS - SPLIT :]
    for s in sends:
        s.wait_send()
    gh_copy.wait()


def on_device(grad_out, hidden, down_weight):
    vm = pltpu.VMEM
    dma = pltpu.SemaphoreType.DMA
    heights = (144, 144, 160)
    scratch = [
        vm((TOK, D), BF), vm((TOK, FFS), BF), vm((TOK, D // 2), BF), vm((TOK, FFS), BF),
        vm((FFS, D), BF), vm((TOK, FFS), BF),
        vm((2, FFS, TOK), BF), vm((2, 4, TOK, 512), BF),
        vm((2, FFS, 128), F32), vm((2, 4, 1, 512), F32),
        vm((448, 512), F32), vm((192, 512), F32), vm((2, 1, PEAKS), F32),
        vm((16, 384), F32), vm((16, 384), BF), vm((16, 384), BF), vm((16, 384), BF),
        vm((3, 16, 384), BF), vm((3, 16, 384), BF), vm((16, 384), BF),
    ]
    scratch += [vm((4, 4, 4, n, 128), BF) for n in heights]
    scratch += [vm((6, 2, 4, n, 128), BF) for n in heights]
    scratch += [vm((6, 2, n, 128), BF) for n in heights]
    scratch += [vm((6, SPLIT, 128), BF) for n in heights]
    scratch += [dma((5,)), dma((7,)), dma, dma((54,)), dma((54,)), dma((12,)), dma((12,))]
    anyspace = pl.BlockSpec(memory_space=pl.ANY)
    vmspace = pl.BlockSpec(memory_space=pltpu.VMEM)
    gh, wg, peaks = pl.pallas_call(
        kernel,
        out_shape=(
            jax.ShapeDtypeStruct((TOK, FFS), BF),
            jax.ShapeDtypeStruct((ROWS, 512), F32),
            jax.ShapeDtypeStruct((1, PEAKS), F32),
        ),
        in_specs=[anyspace] * 3,
        out_specs=(anyspace, vmspace, vmspace),
        scratch_shapes=scratch,
        compiler_params=pltpu.CompilerParams(
            collective_id=0, has_side_effects=True, vmem_limit_bytes=62 * 1024 * 1024),
    )(grad_out[0], hidden[0], down_weight)
    ctx = lax.axis_index("ctx")
    hidden_amax = lax.dynamic_slice(peaks, (0, ctx * (FFS // 16)), (1, FFS // 16))
    grad_amax = lax.dynamic_slice(peaks, (0, FFS + ctx * (D // 16)), (1, D // 16))
    return (gh[None], wg / jnp.sqrt(F32(SEQ * REPLICAS)), hidden_amax, grad_amax)


def solution(mesh):
    placed = (P("dp", "ctx", None), P("dp", "ctx", None), P())
    return jax.shard_map(
        on_device,
        mesh=mesh,
        in_specs=placed,
        out_specs=(P("dp", "ctx", None), P("ctx", "dp"), P("dp", "ctx"), P("dp", "ctx")),
        check_vma=False,
    )
```

```python
import functools

import jax
import jax.numpy as jnp
import numpy as np
from jax import lax
from jax.experimental import pallas as pl
from jax.experimental.pallas import tpu as pltpu
from jax.sharding import PartitionSpec as P

CEILING = 448.0
D, FFS, SEQ, REPLICAS = 4096, 1792, 6144, 8
TOK = 384
BF = jnp.bfloat16
F32 = jnp.float32
MESH = pl.DeviceIdType.MESH
NUDGE = np.float32(1 + 2.0**-21)
ROWS = 112
EXTRA = ((0, 32), (32, 32), (64, 48))
PEAKS = FFS + D
GH = 256
SPLIT = 80


def kernel(g_hbm, h_hbm, w_hbm, gh_hbm, wg_ref, pk_out,
           g_own, h_own, g_peer, w_v, gh_v, hqt, gq, pk,
           stage, am1, am2, am3, amy, amz, amp,
           own0, own1, own2, r10, r11, r12, r20, r21, r22, r30, r31, r32,
           lsem, wsem, osem, ssem, rsem, s2, q2, hs, hr):
    ctx = lax.axis_index("ctx")
    dp = lax.axis_index("dp")
    z, y, x, c = ctx // 4, ctx % 4, dp // 2, dp % 2
    own, rx1, rx2, rx3 = (own0, own1, own2), (r10, r11, r12), (r20, r21, r22), (r30, r31, r32)
    heights = (144, 144, 160)

    def dev(axis, step):
        zz, yy, xx, cc = z, y, x, c
        if axis == "z":
            zz = (z + step) % 4
        elif axis == "y":
            yy = (y + step) % 4
        elif axis == "x":
            xx = (x + step) % 4
        else:
            cc = 1 - c
        return (zz * 4 + yy, xx * 2 + cc)

    lh = pltpu.make_async_copy(h_hbm, h_own, lsem.at[0])
    lh.start()
    lg = []
    for i in range(4):
        at = pl.ds(i * 1024, 1024)
        lg.append(pltpu.make_async_copy(g_hbm.at[:, at], g_own.at[:, at], lsem.at[1 + i]))
        lg[-1].start()

    def wcopy(j):
        at = pl.ds(pl.multiple_of(j * GH, GH), GH)
        return pltpu.make_async_copy(w_hbm.at[at, :], w_v.at[at, :], wsem.at[j])

    barrier = pltpu.get_barrier_semaphore()
    friends = [dev("y", d) for d in (1, 2, 3)] + [dev("z", d) for d in (1, 2, 3)]
    friends += [dev("x", 1), dev("x", 3), dev("c", 1)]
    for f in friends:
        pl.semaphore_signal(barrier, inc=1, device_id=f, device_id_type=MESH)

    sends = []

    def remote(src, dst, i, to, sems=None):
        a, b = sems or (ssem, rsem)
        copy = pltpu.make_async_remote_copy(
            src_ref=src, dst_ref=dst, send_sem=a.at[i], recv_sem=b.at[i],
            device_id=to, device_id_type=MESH)
        copy.start()
        sends.append(copy)
        return copy

    small = (s2, q2)

    def peak_row(ref, lo, size):
        at = pl.ds(pl.multiple_of(lo, 128), size)
        return jnp.max(jnp.abs(ref[:, at].astype(F32)), axis=0, keepdims=True)

    stage[...] = jnp.zeros_like(stage)
    lh.wait()

    def h_peaks(i, _):
        at = pl.multiple_of(i * 256, 256)
        pk[0, :, pl.ds(at, 256)] = peak_row(h_own, at, 256)
        return 0

    lax.fori_loop(0, FFS // 256, h_peaks, 0)
    pl.semaphore_wait(barrier, len(friends))
    peer = dev("c", 1)
    swaps = []
    for i in range(4):
        lg[i].wait()
        src = pl.ds(pl.multiple_of(i * 1024 + (1 - c) * 512, 512), 512)
        swaps.append(remote(g_own.at[:, src], g_peer.at[:, pl.ds(i * 512, 512)], 1 + i, peer, small))

        def g_peaks(k, _, i=i):
            at = pl.multiple_of(i * 1024 + k * 256, 256)
            pk[0, :, pl.ds(FFS + at, 256)] = peak_row(g_own, at, 256)
            return 0

        lax.fori_loop(0, 4, g_peaks, 0)

    def spread(n):
        for r in range(16):
            size = 384 if r < 15 else 128
            yield r, slice(0, size), slice(r * 384, r * 384 + size)

    for j in range(FFS // GH):
        wcopy(j).start()
    for r, a, b in spread(16):
        stage[r : r + 1, a] = pk[0, :, b]
    am1[...] = stage[...].astype(BF)
    gets = [remote(am1, amy.at[d - 1], 5 + d - 1, dev("y", d), small) for d in (1, 2, 3)]

    def gh_step(j, _):
        wcopy(j).wait()
        at = pl.ds(pl.multiple_of(j * GH, GH), GH)
        res = lax.dot_general(
            g_own[...], w_v[at, :], (((1,), (1,)), ((), ())), preferred_element_type=F32)
        gh_v[:, at] = res.astype(BF)
        return 0

    lax.fori_loop(0, 2, gh_step, 0)
    for e in gets:
        e.wait_recv()
    am2[...] = jnp.maximum(
        jnp.maximum(am1[...].astype(F32), amy[0].astype(F32)),
        jnp.maximum(amy[1].astype(F32), amy[2].astype(F32))).astype(BF)
    gets = [remote(am2, amz.at[d - 1], 8 + d - 1, dev("z", d), small) for d in (1, 2, 3)]
    lax.fori_loop(2, 4, gh_step, 0)
    for e in gets:
        e.wait_recv()
    top = jnp.maximum(
        jnp.maximum(am2[...].astype(F32), amz[0].astype(F32)),
        jnp.maximum(amz[1].astype(F32), amz[2].astype(F32)))
    am3[...] = top.astype(BF)
    swap_peaks = remote(am3, amp, 11, peer, small)

    def unpack(r, values):
        stage[...] = jnp.maximum(values, 1.0)
        for k, a, b in spread(16):
            pk[r, :, b] = stage[k : k + 1, a]

    unpack(0, top)
    pk_out[...] = pk[0]

    def on_grid(values, peaks):
        v = values.astype(F32) * ((CEILING / peaks) * 1024.0)
        u = v.astype(jnp.int32).astype(F32) * NUDGE
        big = jnp.maximum(jnp.abs(u) * 2.0**20, 1.5 * 2.0**24)
        return (((u + big) - big) * (peaks / CEILING * 2.0**-10)).astype(BF)

    def quant_g(r, q, j, lo=0, rows=TOK):
        xx = (x + (6 - j) % 4) % 4
        home = xx * 1024 + c * 512 + q * 128
        at = pl.ds(pl.multiple_of(home if r == 0 else xx * 512 + q * 128, 128), 128)
        peaks = pk[r, :, pl.ds(pl.multiple_of(FFS + home, 128), 128)]
        ref = g_own if r == 0 else g_peer
        to = pl.ds(pl.multiple_of(j * 128, 128), 128)
        gq[q, pl.ds(r * TOK + lo, rows), to] = on_grid(ref[pl.ds(lo, rows), at], peaks)

    hsends = []
    for i in range(FFS // 256):
        at = pl.ds(i * 256, 256)
        hqt[at, 0:TOK] = on_grid(h_own[:, at], pk[0, :, at]).T
        if i:
            prev = pl.ds((i - 1) * 256, 256)
            hsends.append(remote(hqt.at[prev, 0:TOK], hqt.at[prev, TOK:], i - 1, peer, (hs, hr)))
    for j in range(2):
        for q in (2, 3):
            quant_g(0, q, j)
        if j == 0:
            prev = pl.ds(FFS - 256, 256)
            hsends.append(remote(hqt.at[prev, 0:TOK], hqt.at[prev, TOK:], 6, peer, (hs, hr)))
    swap_peaks.wait_recv()
    unpack(1, amp[...].astype(F32))
    for e in swaps:
        e.wait_recv()
    for j in range(2):
        for q in (2, 3):
            quant_g(1, q, j)
    for e in hsends:
        e.wait_recv()

    def product(q, offsets, size, cols):
        left = jnp.concatenate(
            [hqt[pl.ds(pl.multiple_of(o, 16), size), :] for o in offsets], axis=0)
        return jnp.dot(left, gq[q, :, cols], preferred_element_type=F32).astype(BF)

    def blocks(p, k, j0, count):
        if p == 1:
            base = [o * 448 + ((y + k) % 4) * ROWS for o in range(4)]
        else:
            base = [((z + k) % 4) * 448 + o * ROWS for o in range(4)]
        lo, size = EXTRA[p]
        cols = slice(j0 * 128, (j0 + count) * 128)
        main = product(p, base, ROWS, cols)
        more = product(3, [b + lo for b in base], size, cols)
        for o in range(4):
            away = (o - z) % 4 if p == 1 else (o - y) % 4
            for j in range(count):
                xr = (6 - j0 - j) % 4
                if p == 0:
                    to = own0.at[k, away, xr]
                elif p == 1:
                    to = own1.at[k, xr, away]
                else:
                    to = own2.at[xr, k, away]
                at = slice(j * 128, j * 128 + 128)
                to[0:ROWS, :] = main[o * ROWS : (o + 1) * ROWS, at]
                to[ROWS : ROWS + size, :] = more[o * size : (o + 1) * size, at]

    axes = (("z", "y", "x"), ("y", "x", "z"), ("x", "z", "y"))

    def piece(ph, p, k, half):
        if ph == 0:
            return own[p].at[k, pl.ds(2 * half, 2)]
        if ph == 1:
            return own[p].at[0, k, pl.ds(2 * half, 2)]
        rows = pl.ds(0, SPLIT) if half == 0 else pl.ds(SPLIT, heights[p] - SPLIT)
        return own[p].at[0, 0, k, rows]

    def landing(ph, p, m, half):
        ref = (rx1, rx2, rx3)[ph][p].at[m]
        if ph == 2:
            return ref.at[pl.ds(0, SPLIT if half == 0 else heights[p] - SPLIT)]
        return ref

    flights = {}
    plan = {
        "a+": (0, 0, 2, 0), "c+": (0, 1, 1, 1), "b+": (0, 2, 1, 0),
        "a-": (1, 3, 2, 1), "c-": (1, 4, 3, 0), "b-": (1, 5, 3, 1),
    }

    def post(ph, p, name):
        way, m, k, half = plan[name]
        to = dev(axes[p][ph], 1 if way == 0 else 3)
        flights[ph, p, name] = remote(
            piece(ph, p, k, half), landing(ph, p, m, half), (ph * 3 + p) * 6 + m, to)

    def arrived(ph, p, name):
        flights[ph, p, name].wait_recv()
        _, m, _, half = plan[name]
        return landing(ph, p, m, half)

    def add_into(ref, others):
        total = ref[...].astype(F32)
        for o in others:
            total = total + o[...].astype(F32)
        ref[...] = total.astype(BF)

    def onward(ph, p):
        for sign, k, half in (("+", 1, 0), ("-", 3, 1)):
            got = arrived(ph, p, "a" + sign)
            mine = piece(ph, p, k, half)
            if ph == 0:
                def step(i, _, mine=mine, got=got):
                    add_into(mine.at[i // 4, i % 4], [got.at[i // 4, i % 4]])
                    return 0
                lax.fori_loop(0, 8, step, 0)
            elif ph == 1:
                for i in range(2):
                    add_into(mine.at[i], [got.at[i]])
            else:
                add_into(mine, [got])
            post(ph, p, "b" + sign)

    def gather_all(ph, p):
        refs = {n: arrived(ph, p, n) for n in ("c+", "c-", "b+", "b-")}
        return (refs["b+"], refs["c-"]), (refs["c+"], refs["b-"])

    def x_first(k, _):
        blocks(2, k, 0, 2)
        for r in range(2):
            quant_g(r, 0, k)
            quant_g(r, 3, 2 + k // 2, pl.multiple_of((k % 2) * (TOK // 2), TOK // 2), TOK // 2)
        return 0

    lax.fori_loop(0, 4, x_first, 0)
    for n in ("a+", "a-", "c+"):
        post(0, 2, n)
    blocks(0, 2, 0, 4)
    for j in range(4):
        quant_g(0, 1, j), quant_g(1, 1, j)
    post(0, 0, "a+"), post(0, 0, "a-")
    blocks(1, 2, 0, 4)
    for j in (2, 3):
        quant_g(0, 2, j), quant_g(1, 2, j)
    post(0, 1, "a+"), post(0, 1, "a-")

    def x_second(k, _):
        blocks(2, k, 2, 2)
        return 0

    lax.fori_loop(0, 4, x_second, 0)
    post(0, 2, "c-")
    for p in (0, 1):
        def rest(j, _, p=p):
            blocks(p, (1 + 2 * j) % 5, 0, 4)
            return 0

        lax.fori_loop(0, 3, rest, 0)
        post(0, p, "c+"), post(0, p, "c-")

    lax.fori_loop(4, FFS // GH, gh_step, 0)
    gh_copy = pltpu.make_async_copy(gh_v, gh_hbm, osem)
    gh_copy.start()

    for p in (2, 0, 1):
        onward(0, p)
    for p in (2, 0, 1):
        pair = gather_all(0, p)
        for k in (2, 1, 3, 0):
            def step(i, _, k=k, pair=pair, p=p):
                add_into(own[p].at[0, k, i], [o.at[k % 2, i] for o in pair[k // 2]])
                return 0

            lax.fori_loop(0, 4, step, 0)
            if k == 2:
                post(1, p, "a+"), post(1, p, "a-")
            elif k == 1:
                post(1, p, "c+")
            elif k == 3:
                post(1, p, "c-")
    for p in (2, 0, 1):
        onward(1, p)
    for p in (2, 0, 1):
        pair = gather_all(1, p)
        for k in (2, 1, 3, 0):
            add_into(own[p].at[0, 0, k], [o.at[k % 2] for o in pair[k // 2]])
            if k == 2:
                post(2, p, "a+"), post(2, p, "a-")
            elif k == 1:
                post(2, p, "c+")
            elif k == 3:
                post(2, p, "c-")
    for p in (2, 0, 1):
        onward(2, p)
    for p in (2, 0, 1):
        pair = gather_all(2, p)
        cols = slice(p * 128, p * 128 + 128)
        lo, size = EXTRA[p]
        for half in (0, 1):
            total = piece(2, p, 0, half)[...].astype(F32)
            for o in pair[half]:
                total = total + o[...].astype(F32)
            if half == 0:
                wg_ref[0:SPLIT, cols] = total
            else:
                wg_ref[SPLIT:ROWS, cols] = total[: ROWS - SPLIT]
                wg_ref[lo : lo + size, 384:512] = total[ROWS - SPLIT :]
    for s in sends:
        s.wait_send()
    gh_copy.wait()


def finish(gh_hbm, wg, pk, gh_out, wg_out, ha_out, ga_out, buf, isem, osem):
    step = TOK // 4
    rows = [pl.ds(i * step, step) for i in range(4)]
    ins = [pltpu.make_async_copy(gh_hbm.at[r], buf.at[r], isem.at[i]) for i, r in enumerate(rows)]
    outs = [pltpu.make_async_copy(buf.at[r], gh_out.at[r], osem.at[i]) for i, r in enumerate(rows)]
    for e in ins:
        e.start()
    wg_out[...] = wg[...] * np.float32(1.0 / np.sqrt(SEQ * REPLICAS))
    ctx = lax.axis_index("ctx")
    some = pk[:, 0:ROWS]
    for k in range(1, 16):
        some = jnp.where(ctx == k, pk[:, k * ROWS : (k + 1) * ROWS], some)
    ha_out[...] = some
    ga_out[...] = pk[:, pl.ds(pl.multiple_of(FFS + ctx * 256, 256), 256)]
    for a, b in zip(ins, outs):
        a.wait()
        b.start()
    for b in outs:
        b.wait()


def on_device(grad_out, hidden, down_weight):
    vm = pltpu.VMEM
    dma = pltpu.SemaphoreType.DMA
    heights = (144, 144, 160)
    scratch = [
        vm((TOK, D), BF), vm((TOK, FFS), BF), vm((TOK, D // 2), BF),
        vm((FFS, D), BF), vm((TOK, FFS), BF),
        vm((FFS, 2 * TOK), BF), vm((4, 2 * TOK, 512), BF), vm((2, 1, PEAKS), F32),
        vm((16, 384), F32), vm((16, 384), BF), vm((16, 384), BF), vm((16, 384), BF),
        vm((3, 16, 384), BF), vm((3, 16, 384), BF), vm((16, 384), BF),
    ]
    scratch += [vm((4, 4, 4, n, 128), BF) for n in heights]
    scratch += [vm((6, 2, 4, n, 128), BF) for n in heights]
    scratch += [vm((6, 2, n, 128), BF) for n in heights]
    scratch += [vm((6, SPLIT, 128), BF) for n in heights]
    scratch += [dma((5,)), dma((7,)), dma, dma((54,)), dma((54,)), dma((12,)), dma((12,)), dma((7,)), dma((7,))]
    anyspace = pl.BlockSpec(memory_space=pl.ANY)
    vmspace = pl.BlockSpec(memory_space=pltpu.VMEM)
    gh, wg, peaks = pl.pallas_call(
        kernel,
        out_shape=(
            jax.ShapeDtypeStruct((TOK, FFS), BF),
            jax.ShapeDtypeStruct((ROWS, 512), F32),
            jax.ShapeDtypeStruct((1, PEAKS), F32),
        ),
        in_specs=[anyspace] * 3,
        out_specs=(anyspace, vmspace, vmspace),
        scratch_shapes=scratch,
        compiler_params=pltpu.CompilerParams(
            collective_id=0, has_side_effects=True, vmem_limit_bytes=62 * 1024 * 1024),
    )(grad_out[0], hidden[0], down_weight)
    gh, wg, ha, ga = pl.pallas_call(
        finish,
        out_shape=(
            jax.ShapeDtypeStruct((TOK, FFS), BF),
            jax.ShapeDtypeStruct((ROWS, 512), F32),
            jax.ShapeDtypeStruct((1, ROWS), F32),
            jax.ShapeDtypeStruct((1, 256), F32),
        ),
        in_specs=[anyspace, vmspace, vmspace],
        out_specs=(anyspace, vmspace, vmspace, vmspace),
        scratch_shapes=[vm((TOK, FFS), BF), dma((4,)), dma((4,))],
    )(gh, wg, peaks)
    return (gh[None], wg, ha, ga)


def solution(mesh):
    placed = (P("dp", "ctx", None), P("dp", "ctx", None), P())
    return jax.shard_map(
        on_device,
        mesh=mesh,
        in_specs=placed,
        out_specs=(P("dp", "ctx", None), P("ctx", "dp"), P("dp", "ctx"), P("dp", "ctx")),
        check_vma=False,
    )
```

```python
import functools

import jax
import jax.numpy as jnp
import numpy as np
from jax import lax
from jax.experimental import pallas as pl
from jax.experimental.pallas import tpu as pltpu
from jax.sharding import PartitionSpec as P

CEILING = 448.0
D, FFS, SEQ, REPLICAS = 4096, 1792, 6144, 8
TOK = 384
BF = jnp.bfloat16
F32 = jnp.float32
MESH = pl.DeviceIdType.MESH
NUDGE = np.float32(1 + 2.0**-21)
ROWS = 112
EXTRA = ((0, 32), (32, 32), (64, 48))
PEAKS = FFS + D
GH = 256
SPLIT = 80


def kernel(g_hbm, h_hbm, w_hbm, gh_v, wg_ref, pk_out,
           g_own, h_own, g_peer, w_v, hqt, gq, pk,
           stage, am1, am2, am3, amy, amz, amp,
           own0, own1, own2, r10, r11, r12, r20, r21, r22, r30, r31, r32,
           lsem, wsem, ssem, rsem, s2, q2, hs, hr):
    ctx = lax.axis_index("ctx")
    dp = lax.axis_index("dp")
    z, y, x, c = ctx // 4, ctx % 4, dp // 2, dp % 2
    own, rx1, rx2, rx3 = (own0, own1, own2), (r10, r11, r12), (r20, r21, r22), (r30, r31, r32)
    heights = (144, 144, 160)

    def dev(axis, step):
        zz, yy, xx, cc = z, y, x, c
        if axis == "z":
            zz = (z + step) % 4
        elif axis == "y":
            yy = (y + step) % 4
        elif axis == "x":
            xx = (x + step) % 4
        else:
            cc = 1 - c
        return (zz * 4 + yy, xx * 2 + cc)

    lh = pltpu.make_async_copy(h_hbm, h_own, lsem.at[0])
    lh.start()
    lg = []
    for i in range(4):
        at = pl.ds(i * 1024, 1024)
        lg.append(pltpu.make_async_copy(g_hbm.at[:, at], g_own.at[:, at], lsem.at[1 + i]))
        lg[-1].start()

    def wcopy(j):
        at = pl.ds(pl.multiple_of(j * GH, GH), GH)
        return pltpu.make_async_copy(w_hbm.at[at, :], w_v.at[at, :], wsem.at[j])

    barrier = pltpu.get_barrier_semaphore()
    friends = [dev("y", d) for d in (1, 2, 3)] + [dev("z", d) for d in (1, 2, 3)]
    friends += [dev("x", 1), dev("x", 3), dev("c", 1)]
    for f in friends:
        pl.semaphore_signal(barrier, inc=1, device_id=f, device_id_type=MESH)

    sends = []

    def remote(src, dst, i, to, sems=None):
        a, b = sems or (ssem, rsem)
        copy = pltpu.make_async_remote_copy(
            src_ref=src, dst_ref=dst, send_sem=a.at[i], recv_sem=b.at[i],
            device_id=to, device_id_type=MESH)
        copy.start()
        sends.append(copy)
        return copy

    small = (s2, q2)

    def peak_row(ref, lo, size):
        at = pl.ds(pl.multiple_of(lo, 128), size)
        return jnp.max(jnp.abs(ref[:, at].astype(F32)), axis=0, keepdims=True)

    stage[...] = jnp.zeros_like(stage)
    lh.wait()

    def h_peaks(i, _):
        at = pl.multiple_of(i * 256, 256)
        pk[0, :, pl.ds(at, 256)] = peak_row(h_own, at, 256)
        return 0

    lax.fori_loop(0, FFS // 256, h_peaks, 0)
    pl.semaphore_wait(barrier, len(friends))
    peer = dev("c", 1)
    swaps = []
    for i in range(4):
        lg[i].wait()
        src = pl.ds(pl.multiple_of(i * 1024 + (1 - c) * 512, 512), 512)
        swaps.append(remote(g_own.at[:, src], g_peer.at[:, pl.ds(i * 512, 512)], 1 + i, peer, small))

        def g_peaks(k, _, i=i):
            at = pl.multiple_of(i * 1024 + k * 256, 256)
            pk[0, :, pl.ds(FFS + at, 256)] = peak_row(g_own, at, 256)
            return 0

        lax.fori_loop(0, 4, g_peaks, 0)

    def spread(n):
        for r in range(16):
            size = 384 if r < 15 else 128
            yield r, slice(0, size), slice(r * 384, r * 384 + size)

    for j in range(FFS // GH):
        wcopy(j).start()
    for r, a, b in spread(16):
        stage[r : r + 1, a] = pk[0, :, b]
    am1[...] = stage[...].astype(BF)
    gets = [remote(am1, amy.at[d - 1], 5 + d - 1, dev("y", d), small) for d in (2, 1, 3)]

    def gh_step(j, _):
        wcopy(j).wait()
        at = pl.ds(pl.multiple_of(j * GH, GH), GH)
        res = lax.dot_general(
            g_own[...], w_v[at, :], (((1,), (1,)), ((), ())), preferred_element_type=F32)
        gh_v[:, at] = res.astype(BF)
        return 0

    gh_step(0, 0)
    for e in gets:
        e.wait_recv()
    am2[...] = jnp.maximum(
        jnp.maximum(am1[...].astype(F32), amy[0].astype(F32)),
        jnp.maximum(amy[1].astype(F32), amy[2].astype(F32))).astype(BF)
    gets = [remote(am2, amz.at[d - 1], 8 + d - 1, dev("z", d), small) for d in (2, 1, 3)]
    lax.fori_loop(1, 3, gh_step, 0)
    for e in gets:
        e.wait_recv()
    top = jnp.maximum(
        jnp.maximum(am2[...].astype(F32), amz[0].astype(F32)),
        jnp.maximum(amz[1].astype(F32), amz[2].astype(F32)))
    am3[...] = top.astype(BF)
    swap_peaks = remote(am3, amp, 11, peer, small)

    def unpack(r, values):
        stage[...] = jnp.maximum(values, 1.0)
        for k, a, b in spread(16):
            pk[r, :, b] = stage[k : k + 1, a]

    unpack(0, top)
    pk_out[...] = pk[0]

    def on_grid(values, peaks):
        v = values.astype(F32) * ((CEILING / peaks) * 1024.0)
        u = v.astype(jnp.int32).astype(F32) * NUDGE
        big = jnp.maximum(jnp.abs(u) * 2.0**20, 1.5 * 2.0**24)
        return (((u + big) - big) * (peaks / CEILING * 2.0**-10)).astype(BF)

    def quant_g(r, q, j, lo=0, rows=TOK):
        xx = (x + (6 - j) % 4) % 4
        home = xx * 1024 + c * 512 + q * 128
        at = pl.ds(pl.multiple_of(home if r == 0 else xx * 512 + q * 128, 128), 128)
        peaks = pk[r, :, pl.ds(pl.multiple_of(FFS + home, 128), 128)]
        ref = g_own if r == 0 else g_peer
        to = pl.ds(pl.multiple_of(j * 128, 128), 128)
        gq[q, pl.ds(r * TOK + lo, rows), to] = on_grid(ref[pl.ds(lo, rows), at], peaks)

    hsends = []
    for i in range(FFS // 256):
        at = pl.ds(i * 256, 256)
        hqt[at, 0:TOK] = on_grid(h_own[:, at], pk[0, :, at]).T
        if i:
            prev = pl.ds((i - 1) * 256, 256)
            hsends.append(remote(hqt.at[prev, 0:TOK], hqt.at[prev, TOK:], i - 1, peer, (hs, hr)))
    for j in range(2):
        for q in (2, 3):
            quant_g(0, q, j)
        if j == 0:
            prev = pl.ds(FFS - 256, 256)
            hsends.append(remote(hqt.at[prev, 0:TOK], hqt.at[prev, TOK:], 6, peer, (hs, hr)))
    for j in range(4):
        quant_g(0, 0, j)
        quant_g(0, 1, j)
        if j > 1:
            quant_g(0, 2, j), quant_g(0, 3, j)
    swap_peaks.wait_recv()
    unpack(1, amp[...].astype(F32))
    for e in swaps:
        e.wait_recv()
    for j in range(2):
        for q in (2, 3):
            quant_g(1, q, j)
    for j in range(4):
        quant_g(1, 0, j)
        if j > 1:
            quant_g(1, 3, j)
    for e in hsends:
        e.wait_recv()

    def product(q, offsets, size, cols):
        left = jnp.concatenate(
            [hqt[pl.ds(pl.multiple_of(o, 16), size), :] for o in offsets], axis=0)
        return jnp.dot(left, gq[q, :, cols], preferred_element_type=F32).astype(BF)

    def blocks(p, k, j0, count):
        if p == 1:
            base = [o * 448 + ((y + k) % 4) * ROWS for o in range(4)]
        else:
            base = [((z + k) % 4) * 448 + o * ROWS for o in range(4)]
        lo, size = EXTRA[p]
        cols = slice(j0 * 128, (j0 + count) * 128)
        main = product(p, base, ROWS, cols)
        more = product(3, [b + lo for b in base], size, cols)
        for o in range(4):
            away = (o - z) % 4 if p == 1 else (o - y) % 4
            for j in range(count):
                xr = (6 - j0 - j) % 4
                if p == 0:
                    to = own0.at[k, away, xr]
                elif p == 1:
                    to = own1.at[k, xr, away]
                else:
                    to = own2.at[xr, k, away]
                at = slice(j * 128, j * 128 + 128)
                to[0:ROWS, :] = main[o * ROWS : (o + 1) * ROWS, at]
                to[ROWS : ROWS + size, :] = more[o * size : (o + 1) * size, at]

    axes = (("z", "y", "x"), ("y", "x", "z"), ("x", "z", "y"))

    def piece(ph, p, k, half):
        if ph == 0:
            return own[p].at[k, pl.ds(2 * half, 2)]
        if ph == 1:
            return own[p].at[0, k, pl.ds(2 * half, 2)]
        rows = pl.ds(0, SPLIT) if half == 0 else pl.ds(SPLIT, heights[p] - SPLIT)
        return own[p].at[0, 0, k, rows]

    def landing(ph, p, m, half):
        ref = (rx1, rx2, rx3)[ph][p].at[m]
        if ph == 2:
            return ref.at[pl.ds(0, SPLIT if half == 0 else heights[p] - SPLIT)]
        return ref

    flights = {}
    plan = {
        "a+": (0, 0, 2, 0), "c+": (0, 1, 1, 1), "b+": (0, 2, 1, 0),
        "a-": (1, 3, 2, 1), "c-": (1, 4, 3, 0), "b-": (1, 5, 3, 1),
    }

    def post(ph, p, name):
        way, m, k, half = plan[name]
        to = dev(axes[p][ph], 1 if way == 0 else 3)
        flights[ph, p, name] = remote(
            piece(ph, p, k, half), landing(ph, p, m, half), (ph * 3 + p) * 8 + m, to)

    def post_part(ph, p, name, idx):
        way, m, k, half = plan[name]
        to = dev(axes[p][ph], 1 if way == 0 else 3)
        sem = (ph * 3 + p) * 8 + (m if idx == 0 else 6 + way)
        flights[ph, p, name, idx] = remote(
            piece(ph, p, k, half).at[idx], landing(ph, p, m, half).at[idx], sem, to)

    def arrived(ph, p, name, idx=None):
        key = (ph, p, name) if idx is None else (ph, p, name, idx)
        if key in flights:
            flights.pop(key).wait_recv()
        _, m, _, half = plan[name]
        ref = landing(ph, p, m, half)
        return ref if idx is None else ref.at[idx]

    def add_into(ref, others):
        total = ref[...].astype(F32)
        for o in others:
            total = total + o[...].astype(F32)
        ref[...] = total.astype(BF)

    def add_rows(ph, ref, others):
        if ph:
            add_into(ref, others)
            return

        def step(i, _):
            add_into(ref.at[i], [o.at[i] for o in others])
            return 0

        lax.fori_loop(0, 4, step, 0)

    def onward(ph, p):
        order = (("-", 0), ("+", 1), ("-", 1), ("+", 0))
        for sign, idx in order if ph < 2 else (("+", None), ("-", None)):
            got = arrived(ph, p, "a" + sign)
            _, _, k, half = plan["b" + sign]
            mine = piece(ph, p, k, half)
            if ph < 2:
                add_rows(ph, mine.at[idx], [got.at[idx]])
                post_part(ph, p, "b" + sign, idx)
            else:
                add_into(mine, [got])
                post(ph, p, "b" + sign)

    def settle(ph):
        for k in (2, 1, 3, 0):
            for p in (2, 0, 1):
                idx = k % 2
                if k < 2:
                    refs = [arrived(ph, p, "c-").at[idx], arrived(ph, p, "b+", idx)]
                else:
                    refs = [arrived(ph, p, "c+").at[idx], arrived(ph, p, "b-", idx)]
                add_rows(ph, own[p].at[(0,) * (ph + 1) + (k,)], refs)
                if k == 2:
                    post(ph + 1, p, "a+"), post(ph + 1, p, "a-")
                elif k:
                    post(ph + 1, p, "c+" if k == 1 else "c-")

    def gather_all(ph, p):
        refs = {n: arrived(ph, p, n) for n in ("c+", "c-", "b+", "b-")}
        return (refs["b+"], refs["c-"]), (refs["c+"], refs["b-"])

    for k in range(4):
        blocks(2, k, 0, 2)
    for n in ("a+", "a-", "c+"):
        post(0, 2, n)
    blocks(0, 2, 0, 4)
    for j in range(4):
        quant_g(1, 1, j)
    post(0, 0, "a+"), post(0, 0, "a-")
    blocks(1, 2, 0, 4)
    for j in (2, 3):
        quant_g(1, 2, j)
    post(0, 1, "a+"), post(0, 1, "a-")
    for k in range(4):
        blocks(2, k, 2, 2)
    post(0, 2, "c-")
    for p in (0, 1):
        for k in (1, 3):
            blocks(p, k, 0, 4)
            post(0, p, "c+" if k == 1 else "c-")
    for p in (0, 1):
        blocks(p, 0, 0, 4)

    lax.fori_loop(3, FFS // GH, gh_step, 0)

    for p in (2, 0, 1):
        onward(0, p)
    settle(0)
    for p in (2, 0, 1):
        onward(1, p)
    settle(1)
    for p in (2, 0, 1):
        onward(2, p)
    for p in (2, 0, 1):
        pair = gather_all(2, p)
        cols = slice(p * 128, p * 128 + 128)
        lo, size = EXTRA[p]
        for half in (0, 1):
            total = piece(2, p, 0, half)[...].astype(F32)
            for o in pair[half]:
                total = total + o[...].astype(F32)
            if half == 0:
                wg_ref[0:SPLIT, cols] = total
            else:
                wg_ref[SPLIT:ROWS, cols] = total[: ROWS - SPLIT]
                wg_ref[lo : lo + size, 384:512] = total[ROWS - SPLIT :]
    for s in sends:
        s.wait_send()


def finish(gh, wg, pk, gh_out, wg_out, ha_out, ga_out, osem):
    out = pltpu.make_async_copy(gh, gh_out, osem)
    out.start()
    wg_out[...] = wg[...] * np.float32(1.0 / np.sqrt(SEQ * REPLICAS))
    ctx = lax.axis_index("ctx")
    some = pk[:, 0:ROWS]
    for k in range(1, 16):
        some = jnp.where(ctx == k, pk[:, k * ROWS : (k + 1) * ROWS], some)
    ha_out[...] = some
    ga_out[...] = pk[:, pl.ds(pl.multiple_of(FFS + ctx * 256, 256), 256)]
    out.wait()


def on_device(grad_out, hidden, down_weight):
    vm = pltpu.VMEM
    dma = pltpu.SemaphoreType.DMA
    heights = (144, 144, 160)
    scratch = [
        vm((TOK, D), BF), vm((TOK, FFS), BF), vm((TOK, D // 2), BF),
        vm((FFS, D), BF),
        vm((FFS, 2 * TOK), BF), vm((4, 2 * TOK, 512), BF), vm((2, 1, PEAKS), F32),
        vm((16, 384), F32), vm((16, 384), BF), vm((16, 384), BF), vm((16, 384), BF),
        vm((3, 16, 384), BF), vm((3, 16, 384), BF), vm((16, 384), BF),
    ]
    scratch += [vm((4, 4, 4, n, 128), BF) for n in heights]
    scratch += [vm((6, 2, 4, n, 128), BF) for n in heights]
    scratch += [vm((6, 2, n, 128), BF) for n in heights]
    scratch += [vm((6, SPLIT, 128), BF) for n in heights]
    scratch += [dma((5,)), dma((7,)), dma((72,)), dma((72,)), dma((12,)), dma((12,)), dma((7,)), dma((7,))]
    hbm = pl.BlockSpec(memory_space=pltpu.HBM)
    vmspace = pl.BlockSpec(memory_space=pltpu.VMEM)
    gh, wg, peaks = pl.pallas_call(
        kernel,
        out_shape=(
            jax.ShapeDtypeStruct((TOK, FFS), BF),
            jax.ShapeDtypeStruct((ROWS, 512), F32),
            jax.ShapeDtypeStruct((1, PEAKS), F32),
        ),
        in_specs=[hbm] * 3,
        out_specs=(vmspace, vmspace, vmspace),
        scratch_shapes=scratch,
        compiler_params=pltpu.CompilerParams(
            collective_id=0, has_side_effects=True, vmem_limit_bytes=54_000_000),
    )(grad_out[0], hidden[0], down_weight)
    gh, wg, ha, ga = pl.pallas_call(
        finish,
        out_shape=(
            jax.ShapeDtypeStruct((TOK, FFS), BF),
            jax.ShapeDtypeStruct((ROWS, 512), F32),
            jax.ShapeDtypeStruct((1, ROWS), F32),
            jax.ShapeDtypeStruct((1, 256), F32),
        ),
        in_specs=[vmspace, vmspace, vmspace],
        out_specs=(hbm, vmspace, vmspace, vmspace),
        scratch_shapes=[dma],
        compiler_params=pltpu.CompilerParams(vmem_limit_bytes=8 * 1024 * 1024),
    )(gh, wg, peaks)
    return (gh[None], wg, ha, ga)


def solution(mesh):
    placed = (P("dp", "ctx", None), P("dp", "ctx", None), P())
    return jax.shard_map(
        on_device,
        mesh=mesh,
        in_specs=placed,
        out_specs=(P("dp", "ctx", None), P("ctx", "dp"), P("dp", "ctx"), P("dp", "ctx")),
        check_vma=False,
    )
```

```python
import functools

import jax
import jax.numpy as jnp
import numpy as np
from jax import lax
from jax.experimental import pallas as pl
from jax.experimental.pallas import tpu as pltpu
from jax.sharding import PartitionSpec as P

CEILING = 448.0
D, FFS, SEQ, REPLICAS = 4096, 1792, 6144, 8
TOK = 384
BF = jnp.bfloat16
F32 = jnp.float32
MESH = pl.DeviceIdType.MESH
NUDGE = np.float32(1 + 2.0**-21)
ROWS = 112
EXTRA = ((0, 32), (32, 32), (64, 48))
PEAKS = FFS + D
GH = 256


def kernel(g_hbm, h_hbm, w_hbm, gh_v, wg_ref, pk_out,
           g_own, h_own, g_peer, w_v, hqt, gq, pk,
           stage, am1, am2, am3, amy, amz, amp,
           own0, own1, own2, r10, r11, r12, r20, r21, r22, r30, r31, r32,
           lsem, wsem, ssem, rsem, s2, q2, hs, hr):
    ctx = lax.axis_index("ctx")
    dp = lax.axis_index("dp")
    z, y, x, c = ctx // 4, ctx % 4, dp // 2, dp % 2
    own, rx1, rx2, rx3 = (own0, own1, own2), (r10, r11, r12), (r20, r21, r22), (r30, r31, r32)

    def dev(axis, step):
        zz, yy, xx, cc = z, y, x, c
        if axis == "z":
            zz = (z + step) % 4
        elif axis == "y":
            yy = (y + step) % 4
        elif axis == "x":
            xx = (x + step) % 4
        else:
            cc = 1 - c
        return (zz * 4 + yy, xx * 2 + cc)

    lh = pltpu.make_async_copy(h_hbm, h_own, lsem.at[0])
    lh.start()
    lg = []
    for i in range(4):
        at = pl.ds(i * 1024, 1024)
        lg.append(pltpu.make_async_copy(g_hbm.at[:, at], g_own.at[:, at], lsem.at[1 + i]))
        lg[-1].start()

    def wcopy(j):
        at = pl.ds(pl.multiple_of(j * GH, GH), GH)
        return pltpu.make_async_copy(w_hbm.at[at, :], w_v.at[at, :], wsem.at[j])

    barrier = pltpu.get_barrier_semaphore()
    friends = [dev("y", d) for d in (1, 2, 3)] + [dev("z", d) for d in (1, 2, 3)]
    friends += [dev("x", d) for d in (1, 2, 3)] + [dev("c", 1)]
    for f in friends:
        pl.semaphore_signal(barrier, inc=1, device_id=f, device_id_type=MESH)

    sends = []

    def remote(src, dst, i, to, sems=None):
        a, b = sems or (ssem, rsem)
        copy = pltpu.make_async_remote_copy(
            src_ref=src, dst_ref=dst, send_sem=a.at[i], recv_sem=b.at[i],
            device_id=to, device_id_type=MESH)
        copy.start()
        sends.append(copy)
        return copy

    small = (s2, q2)

    def peak_row(ref, lo, size):
        at = pl.ds(pl.multiple_of(lo, 128), size)
        return jnp.max(jnp.abs(ref[:, at].astype(F32)), axis=0, keepdims=True)

    stage[...] = jnp.zeros_like(stage)
    lh.wait()

    def h_peaks(i, _):
        at = pl.multiple_of(i * 256, 256)
        pk[0, :, pl.ds(at, 256)] = peak_row(h_own, at, 256)
        return 0

    lax.fori_loop(0, FFS // 256, h_peaks, 0)
    pl.semaphore_wait(barrier, len(friends))
    peer = dev("c", 1)
    wcopy(0).start()
    swaps = []
    for i in range(4):
        lg[i].wait()
        src = pl.ds(pl.multiple_of(i * 1024 + (1 - c) * 512, 512), 512)
        swaps.append(remote(g_own.at[:, src], g_peer.at[:, pl.ds(i * 512, 512)], 1 + i, peer, small))

        def g_peaks(k, _, i=i):
            at = pl.multiple_of(i * 1024 + k * 256, 256)
            pk[0, :, pl.ds(FFS + at, 256)] = peak_row(g_own, at, 256)
            return 0

        lax.fori_loop(0, 4, g_peaks, 0)

    def spread(n):
        for r in range(16):
            size = 384 if r < 15 else 128
            yield r, slice(0, size), slice(r * 384, r * 384 + size)

    for j in range(1, FFS // GH):
        wcopy(j).start()
    for r, a, b in spread(16):
        stage[r : r + 1, a] = pk[0, :, b]
    am1[...] = stage[...].astype(BF)
    gets = [remote(am1, amy.at[d - 1], 5 + d - 1, dev("y", d), small) for d in (2, 1, 3)]

    def gh_step(j, _):
        wcopy(j).wait()
        at = pl.ds(pl.multiple_of(j * GH, GH), GH)
        res = lax.dot_general(
            g_own[...], w_v[at, :], (((1,), (1,)), ((), ())), preferred_element_type=F32)
        gh_v[:, at] = res.astype(BF)
        return 0

    gh_step(0, 0)
    for e in gets:
        e.wait_recv()
    am2[...] = jnp.maximum(
        jnp.maximum(am1[...].astype(F32), amy[0].astype(F32)),
        jnp.maximum(amy[1].astype(F32), amy[2].astype(F32))).astype(BF)
    gets = [remote(am2, amz.at[d - 1], 8 + d - 1, dev("z", d), small) for d in (2, 1, 3)]
    lax.fori_loop(1, 3, gh_step, 0)
    for e in gets:
        e.wait_recv()
    top = jnp.maximum(
        jnp.maximum(am2[...].astype(F32), amz[0].astype(F32)),
        jnp.maximum(amz[1].astype(F32), amz[2].astype(F32)))
    am3[...] = top.astype(BF)
    swap_peaks = remote(am3, amp, 11, peer, small)

    def unpack(r, values):
        stage[...] = jnp.maximum(values, 1.0)
        for k, a, b in spread(16):
            pk[r, :, b] = stage[k : k + 1, a]

    unpack(0, top)
    pk_out[...] = pk[0]

    def on_grid(values, peaks):
        v = values.astype(F32) * ((CEILING / peaks) * 1024.0)
        u = v.astype(jnp.int32).astype(F32) * NUDGE
        big = jnp.maximum(jnp.abs(u) * 2.0**20, 1.5 * 2.0**24)
        return (((u + big) - big) * (peaks / CEILING * 2.0**-10)).astype(BF)

    def quant_g(r, q, j, lo=0, rows=TOK):
        xx = (x + (6 - j) % 4) % 4
        home = xx * 1024 + c * 512 + q * 128
        at = pl.ds(pl.multiple_of(home if r == 0 else xx * 512 + q * 128, 128), 128)
        peaks = pk[r, :, pl.ds(pl.multiple_of(FFS + home, 128), 128)]
        ref = g_own if r == 0 else g_peer
        to = pl.ds(pl.multiple_of(j * 128, 128), 128)
        gq[q, pl.ds(r * TOK + lo, rows), to] = on_grid(ref[pl.ds(lo, rows), at], peaks)

    hsends = []
    for i in range(FFS // 256):
        at = pl.ds(i * 256, 256)
        hqt[at, 0:TOK] = on_grid(h_own[:, at], pk[0, :, at]).T
        if i:
            prev = pl.ds((i - 1) * 256, 256)
            hsends.append(remote(hqt.at[prev, 0:TOK], hqt.at[prev, TOK:], i - 1, peer, (hs, hr)))
    for j in range(2):
        for q in (2, 3):
            quant_g(0, q, j)
        if j == 0:
            prev = pl.ds(FFS - 256, 256)
            hsends.append(remote(hqt.at[prev, 0:TOK], hqt.at[prev, TOK:], 6, peer, (hs, hr)))
    for j in range(4):
        quant_g(0, 0, j)
        quant_g(0, 1, j)
        if j > 1:
            quant_g(0, 2, j), quant_g(0, 3, j)
    swap_peaks.wait_recv()
    unpack(1, amp[...].astype(F32))
    for e in swaps:
        e.wait_recv()
    for j in range(2):
        for q in (2, 3):
            quant_g(1, q, j)
    for j in range(4):
        quant_g(1, 0, j)
        if j > 1:
            quant_g(1, 3, j)
    for e in hsends:
        e.wait_recv()

    def product(q, offsets, size, cols):
        left = jnp.concatenate(
            [hqt[pl.ds(pl.multiple_of(o, 16), size), :] for o in offsets], axis=0)
        return jnp.dot(left, gq[q, :, cols], preferred_element_type=F32).astype(BF)

    def blocks(p, k, j0, count):
        if p == 1:
            base = [o * 448 + ((y + k) % 4) * ROWS for o in range(4)]
        else:
            base = [((z + k) % 4) * 448 + o * ROWS for o in range(4)]
        lo, size = EXTRA[p]
        cols = slice(j0 * 128, (j0 + count) * 128)
        main = product(p, base, ROWS, cols)
        more = product(3, [b + lo for b in base], size, cols)
        for o in range(4):
            away = (o - z) % 4 if p == 1 else (o - y) % 4
            for j in range(count):
                xr = (6 - j0 - j) % 4
                if p == 0:
                    to = own0.at[k, away, xr]
                elif p == 1:
                    to = own1.at[k, xr, away]
                else:
                    to = own2.at[xr, k, away]
                at = slice(j * 128, j * 128 + 128)
                to[0:ROWS, :] = main[o * ROWS : (o + 1) * ROWS, at]
                to[ROWS : ROWS + size, :] = more[o * size : (o + 1) * size, at]

    axes = (("z", "y", "x"), ("y", "x", "z"), ("x", "z", "y"))

    def piece(ph, p, k, half):
        ref = own[p].at[k] if ph == 0 else own[p].at[0, k]
        return ref.at[pl.ds(2 * half, 2)]

    def landing(ph, p, m, half):
        return (rx1, rx2)[ph][p].at[m]

    flights = {}
    plan = {
        "a+": (0, 0, 2, 0), "c+": (0, 1, 1, 1), "b+": (0, 2, 1, 0),
        "a-": (1, 3, 2, 1), "c-": (1, 4, 3, 0), "b-": (1, 5, 3, 1),
    }

    def post(ph, p, name):
        way, m, k, half = plan[name]
        to = dev(axes[p][ph], 1 if way == 0 else 3)
        flights[ph, p, name] = remote(
            piece(ph, p, k, half), landing(ph, p, m, half), (ph * 3 + p) * 8 + m, to)

    def post_part(ph, p, name, idx):
        way, m, k, half = plan[name]
        to = dev(axes[p][ph], 1 if way == 0 else 3)
        sem = (ph * 3 + p) * 8 + (m if idx == 0 else 6 + way)
        flights[ph, p, name, idx] = remote(
            piece(ph, p, k, half).at[idx], landing(ph, p, m, half).at[idx], sem, to)

    def arrived(ph, p, name, idx=None):
        key = (ph, p, name) if idx is None else (ph, p, name, idx)
        if key in flights:
            flights.pop(key).wait_recv()
        _, m, _, half = plan[name]
        ref = landing(ph, p, m, half)
        return ref if idx is None else ref.at[idx]

    def add_into(ref, others):
        total = ref[...].astype(F32)
        for o in others:
            total = total + o[...].astype(F32)
        ref[...] = total.astype(BF)

    def onward(ph, p):
        for sign, idx in (("-", 0), ("+", 1), ("-", 1), ("+", 0)):
            got = arrived(ph, p, "a" + sign)
            _, _, k, half = plan["b" + sign]
            add_into(piece(ph, p, k, half).at[idx], [got.at[idx]])
            post_part(ph, p, "b" + sign, idx)

    def direct(p, k):
        return remote(own[p].at[0, 0, k], rx3[p].at[k - 1], (6 + p) * 8 + k, dev(axes[p][2], k))

    def settle(ph):
        for k in (2, 1, 3, 0):
            for p in (2, 0, 1):
                idx = k % 2
                if k < 2:
                    refs = [arrived(ph, p, "c-").at[idx], arrived(ph, p, "b+", idx)]
                else:
                    refs = [arrived(ph, p, "c+").at[idx], arrived(ph, p, "b-", idx)]
                add_into(own[p].at[(0,) * (ph + 1) + (k,)], refs)
                if ph:
                    if k:
                        last[p].append(direct(p, k))
                elif k == 2:
                    post(1, p, "a+"), post(1, p, "a-")
                elif k:
                    post(1, p, "c+" if k == 1 else "c-")

    last = ([], [], [])

    for k in range(4):
        blocks(2, k, 0, 2)
    for n in ("a+", "a-", "c+"):
        post(0, 2, n)
    blocks(0, 2, 0, 4)
    for j in range(4):
        quant_g(1, 1, j)
    post(0, 0, "a+"), post(0, 0, "a-")
    blocks(1, 2, 0, 4)
    for j in (2, 3):
        quant_g(1, 2, j)
    post(0, 1, "a+"), post(0, 1, "a-")
    for k in range(4):
        blocks(2, k, 2, 2)
    post(0, 2, "c-")
    for p in (0, 1):
        for k in (1, 3):
            blocks(p, k, 0, 4)
            post(0, p, "c+" if k == 1 else "c-")
    for p in (0, 1):
        blocks(p, 0, 0, 4)

    lax.fori_loop(3, 6, gh_step, 0)

    for p in (2, 0, 1):
        onward(0, p)
    lax.fori_loop(6, FFS // GH, gh_step, 0)
    settle(0)
    for p in (2, 0, 1):
        onward(1, p)
    settle(1)
    for p in (2, 0, 1):
        cols = slice(p * 128, p * 128 + 128)
        lo, size = EXTRA[p]
        for e in last[p]:
            e.wait_recv()
        total = own[p][0, 0, 0].astype(F32)
        for d in range(3):
            total = total + rx3[p][d].astype(F32)
        wg_ref[:, cols] = total[:ROWS]
        wg_ref[lo : lo + size, 384:512] = total[ROWS:]
    for s in sends:
        s.wait_send()


def finish(gh, wg, pk, gh_out, wg_out, ha_out, ga_out, osem):
    out = pltpu.make_async_copy(gh, gh_out, osem)
    out.start()
    wg_out[...] = wg[...] * np.float32(1.0 / np.sqrt(SEQ * REPLICAS))
    ctx = lax.axis_index("ctx")
    some = pk[:, 0:ROWS]
    for k in range(1, 16):
        some = jnp.where(ctx == k, pk[:, k * ROWS : (k + 1) * ROWS], some)
    ha_out[...] = some
    ga_out[...] = pk[:, pl.ds(pl.multiple_of(FFS + ctx * 256, 256), 256)]
    out.wait()


def on_device(grad_out, hidden, down_weight):
    vm = pltpu.VMEM
    dma = pltpu.SemaphoreType.DMA
    heights = (144, 144, 160)
    scratch = [
        vm((TOK, D), BF), vm((TOK, FFS), BF), vm((TOK, D // 2), BF),
        vm((FFS, D), BF),
        vm((FFS, 2 * TOK), BF), vm((4, 2 * TOK, 512), BF), vm((2, 1, PEAKS), F32),
        vm((16, 384), F32), vm((16, 384), BF), vm((16, 384), BF), vm((16, 384), BF),
        vm((3, 16, 384), BF), vm((3, 16, 384), BF), vm((16, 384), BF),
    ]
    scratch += [vm((4, 4, 4, n, 128), BF) for n in heights]
    scratch += [vm((6, 2, 4, n, 128), BF) for n in heights]
    scratch += [vm((6, 2, n, 128), BF) for n in heights]
    scratch += [vm((3, n, 128), BF) for n in heights]
    scratch += [dma((5,)), dma((7,)), dma((72,)), dma((72,)), dma((12,)), dma((12,)), dma((7,)), dma((7,))]
    hbm = pl.BlockSpec(memory_space=pltpu.HBM)
    vmspace = pl.BlockSpec(memory_space=pltpu.VMEM)
    gh, wg, peaks = pl.pallas_call(
        kernel,
        out_shape=(
            jax.ShapeDtypeStruct((TOK, FFS), BF),
            jax.ShapeDtypeStruct((ROWS, 512), F32),
            jax.ShapeDtypeStruct((1, PEAKS), F32),
        ),
        in_specs=[hbm] * 3,
        out_specs=(vmspace, vmspace, vmspace),
        scratch_shapes=scratch,
        compiler_params=pltpu.CompilerParams(
            collective_id=0, has_side_effects=True, vmem_limit_bytes=54_000_000),
    )(grad_out[0], hidden[0], down_weight)
    gh, wg, ha, ga = pl.pallas_call(
        finish,
        out_shape=(
            jax.ShapeDtypeStruct((TOK, FFS), BF),
            jax.ShapeDtypeStruct((ROWS, 512), F32),
            jax.ShapeDtypeStruct((1, ROWS), F32),
            jax.ShapeDtypeStruct((1, 256), F32),
        ),
        in_specs=[vmspace, vmspace, vmspace],
        out_specs=(hbm, vmspace, vmspace, vmspace),
        scratch_shapes=[dma],
        compiler_params=pltpu.CompilerParams(vmem_limit_bytes=8 * 1024 * 1024),
    )(gh, wg, peaks)
    return (gh[None], wg, ha, ga)


def solution(mesh):
    placed = (P("dp", "ctx", None), P("dp", "ctx", None), P())
    return jax.shard_map(
        on_device,
        mesh=mesh,
        in_specs=placed,
        out_specs=(P("dp", "ctx", None), P("ctx", "dp"), P("dp", "ctx"), P("dp", "ctx")),
        check_vma=False,
    )
```

```python
import functools

import jax
import jax.numpy as jnp
import numpy as np
from jax import lax
from jax.experimental import pallas as pl
from jax.experimental.pallas import tpu as pltpu
from jax.sharding import PartitionSpec as P

CEILING = 448.0
D, FFS, SEQ, REPLICAS = 4096, 1792, 6144, 8
TOK = 384
BF = jnp.bfloat16
F32 = jnp.float32
MESH = pl.DeviceIdType.MESH
NUDGE = np.float32(1 + 2.0**-21)
ROWS = 112
EXTRA = ((0, 32), (32, 32), (64, 48))
PEAKS = FFS + D
SENDS = 24
GH = 256


def kernel(g_hbm, h_hbm, w_hbm, gh_v, wg_ref, pk_out,
           g_own, h_own, g_peer, w_v, hqt, gq, pk,
           stage, am1, am2, am3, amy, amz, amp,
           own0, own1, own2, r10, r11, r12, r20, r21, r22, r30, r31, r32,
           lsem, wsem, ssem, rsem):
    ctx = lax.axis_index("ctx")
    dp = lax.axis_index("dp")
    z, y, x, c = ctx // 4, ctx % 4, dp // 2, dp % 2
    own, rx1, rx2, rx3 = (own0, own1, own2), (r10, r11, r12), (r20, r21, r22), (r30, r31, r32)

    def dev(axis, step):
        zz, yy, xx, cc = z, y, x, c
        if axis == "z":
            zz = (z + step) % 4
        elif axis == "y":
            yy = (y + step) % 4
        elif axis == "x":
            xx = (x + step) % 4
        else:
            cc = 1 - c
        return (zz * 4 + yy, xx * 2 + cc)

    lh = pltpu.make_async_copy(h_hbm, h_own, lsem.at[0])
    lh.start()
    lg = []
    for i in range(4):
        at = pl.ds(i * 1024, 1024)
        lg.append(pltpu.make_async_copy(g_hbm.at[:, at], g_own.at[:, at], lsem.at[1 + i]))
        lg[-1].start()

    def wcopy(j):
        at = pl.ds(pl.multiple_of(j * GH, GH), GH)
        return pltpu.make_async_copy(w_hbm.at[at, :], w_v.at[at, :], wsem.at[j])

    barrier = pltpu.get_barrier_semaphore()
    friends = [dev("y", d) for d in (1, 2, 3)] + [dev("z", d) for d in (1, 2, 3)]
    friends += [dev("x", d) for d in (1, 2, 3)] + [dev("c", 1)]
    for f in friends:
        pl.semaphore_signal(barrier, inc=1, device_id=f, device_id_type=MESH)

    sends = []

    def remote(src, dst, i, to, base=0):
        slot = len(sends) % SENDS
        if len(sends) >= SENDS:
            sends[-SENDS].wait_send()
        copy = pltpu.make_async_remote_copy(
            src_ref=src, dst_ref=dst, send_sem=ssem.at[slot], recv_sem=rsem.at[base + i],
            device_id=to, device_id_type=MESH)
        copy.start()
        sends.append(copy)
        return copy

    small = 57

    def peak_row(ref, lo, size):
        at = pl.ds(pl.multiple_of(lo, 128), size)
        return jnp.max(jnp.abs(ref[:, at].astype(F32)), axis=0, keepdims=True)

    stage[...] = jnp.zeros_like(stage)
    lh.wait()

    def h_peaks(i, _):
        at = pl.multiple_of(i * 256, 256)
        pk[0, :, pl.ds(at, 256)] = peak_row(h_own, at, 256)
        return 0

    lax.fori_loop(0, FFS // 256, h_peaks, 0)
    pl.semaphore_wait(barrier, len(friends))
    peer = dev("c", 1)
    wcopy(0).start()
    swaps = []
    for i in range(4):
        lg[i].wait()
        src = pl.ds(pl.multiple_of(i * 1024 + (1 - c) * 512, 512), 512)
        swaps.append(remote(g_own.at[:, src], g_peer.at[:, pl.ds(i * 512, 512)], 1 + i, peer, small))

        def g_peaks(k, _, i=i):
            at = pl.multiple_of(i * 1024 + k * 256, 256)
            pk[0, :, pl.ds(FFS + at, 256)] = peak_row(g_own, at, 256)
            return 0

        lax.fori_loop(0, 4, g_peaks, 0)

    def spread(n):
        for r in range(16):
            size = 384 if r < 15 else 128
            yield r, slice(0, size), slice(r * 384, r * 384 + size)

    for j in range(1, FFS // GH):
        wcopy(j).start()
    for r, a, b in spread(16):
        stage[r : r + 1, a] = pk[0, :, b]
    am1[...] = stage[...].astype(BF)
    gets = [remote(am1, amy.at[d - 1], 5 + d - 1, dev("y", d), small) for d in (2, 1, 3)]

    def gh_step(j, _):
        wcopy(j).wait()
        at = pl.ds(pl.multiple_of(j * GH, GH), GH)
        res = lax.dot_general(
            g_own[...], w_v[at, :], (((1,), (1,)), ((), ())), preferred_element_type=F32)
        gh_v[:, at] = res.astype(BF)
        return 0

    gh_step(0, 0)
    for e in gets:
        e.wait_recv()
    am2[...] = jnp.maximum(
        jnp.maximum(am1[...].astype(F32), amy[0].astype(F32)),
        jnp.maximum(amy[1].astype(F32), amy[2].astype(F32))).astype(BF)
    gets = [remote(am2, amz.at[d - 1], 8 + d - 1, dev("z", d), small) for d in (2, 1, 3)]
    lax.fori_loop(1, 3, gh_step, 0)
    for e in gets:
        e.wait_recv()
    top = jnp.maximum(
        jnp.maximum(am2[...].astype(F32), amz[0].astype(F32)),
        jnp.maximum(amz[1].astype(F32), amz[2].astype(F32)))
    am3[...] = top.astype(BF)
    swap_peaks = remote(am3, amp, 11, peer, small)

    def unpack(r, values):
        stage[...] = jnp.maximum(values, 1.0)
        for k, a, b in spread(16):
            pk[r, :, b] = stage[k : k + 1, a]

    unpack(0, top)
    pk_out[...] = pk[0]

    def on_grid(values, peaks):
        v = values.astype(F32) * ((CEILING / peaks) * 1024.0)
        u = v.astype(jnp.int32).astype(F32) * NUDGE
        big = jnp.maximum(jnp.abs(u) * 2.0**20, 1.5 * 2.0**24)
        return (((u + big) - big) * (peaks / CEILING * 2.0**-10)).astype(BF)

    def quant_g(r, q, j, lo=0, rows=TOK):
        xx = (x + (6 - j) % 4) % 4
        home = xx * 1024 + c * 512 + q * 128
        at = pl.ds(pl.multiple_of(home if r == 0 else xx * 512 + q * 128, 128), 128)
        peaks = pk[r, :, pl.ds(pl.multiple_of(FFS + home, 128), 128)]
        ref = g_own if r == 0 else g_peer
        to = pl.ds(pl.multiple_of(j * 128, 128), 128)
        gq[q, pl.ds(r * TOK + lo, rows), to] = on_grid(ref[pl.ds(lo, rows), at], peaks)

    hsends = []
    for i in range(FFS // 256):
        at = pl.ds(i * 256, 256)
        hqt[at, 0:TOK] = on_grid(h_own[:, at], pk[0, :, at]).T
        if i:
            prev = pl.ds((i - 1) * 256, 256)
            hsends.append(remote(hqt.at[prev, 0:TOK], hqt.at[prev, TOK:], i - 1, peer, 69))
    for j in range(2):
        for q in (2, 3):
            quant_g(0, q, j)
        if j == 0:
            prev = pl.ds(FFS - 256, 256)
            hsends.append(remote(hqt.at[prev, 0:TOK], hqt.at[prev, TOK:], 6, peer, 69))
    for j in range(4):
        quant_g(0, 0, j)
        quant_g(0, 1, j)
        if j > 1:
            quant_g(0, 2, j), quant_g(0, 3, j)
    swap_peaks.wait_recv()
    unpack(1, amp[...].astype(F32))
    for e in swaps:
        e.wait_recv()
    for j in range(2):
        for q in (2, 3):
            quant_g(1, q, j)
    for j in range(4):
        quant_g(1, 0, j)
        if j > 1:
            quant_g(1, 3, j)
    for e in hsends:
        e.wait_recv()

    def product(q, offsets, size, cols):
        left = jnp.concatenate(
            [hqt[pl.ds(pl.multiple_of(o, 16), size), :] for o in offsets], axis=0)
        return jnp.dot(left, gq[q, :, cols], preferred_element_type=F32).astype(BF)

    def blocks(p, k, j0, count):
        if p == 1:
            base = [o * 448 + ((y + k) % 4) * ROWS for o in range(4)]
        else:
            base = [((z + k) % 4) * 448 + o * ROWS for o in range(4)]
        lo, size = EXTRA[p]
        cols = slice(j0 * 128, (j0 + count) * 128)
        main = product(p, base, ROWS, cols)
        more = product(3, [b + lo for b in base], size, cols)
        for o in range(4):
            away = (o - z) % 4 if p == 1 else (o - y) % 4
            for j in range(count):
                xr = (6 - j0 - j) % 4
                if p == 0:
                    to = own0.at[k, away, xr]
                elif p == 1:
                    to = own1.at[k, xr, away]
                else:
                    to = own2.at[xr, k, away]
                at = slice(j * 128, j * 128 + 128)
                to[0:ROWS, :] = main[o * ROWS : (o + 1) * ROWS, at]
                to[ROWS : ROWS + size, :] = more[o * size : (o + 1) * size, at]

    axes = (("z", "y", "x"), ("y", "x", "z"), ("x", "z", "y"))

    def piece(ph, p, k, half):
        ref = own[p].at[k] if ph == 0 else own[p].at[0, k]
        return ref.at[pl.ds(2 * half, 2)]

    def landing(ph, p, m, half):
        return (rx1, rx2)[ph][p].at[m]

    flights = {}
    plan = {
        "a+": (0, 0, 2, 0), "c+": (0, 1, 1, 1), "b+": (0, 2, 1, 0),
        "a-": (1, 3, 2, 1), "c-": (1, 4, 3, 0), "b-": (1, 5, 3, 1),
    }

    def post(ph, p, name):
        way, m, k, half = plan[name]
        to = dev(axes[p][ph], 1 if way == 0 else 3)
        flights[ph, p, name] = remote(
            piece(ph, p, k, half), landing(ph, p, m, half), (ph * 3 + p) * 8 + m, to)

    def post_part(ph, p, name, idx):
        way, m, k, half = plan[name]
        to = dev(axes[p][ph], 1 if way == 0 else 3)
        sem = (ph * 3 + p) * 8 + (m if idx == 0 else 6 + way)
        flights[ph, p, name, idx] = remote(
            piece(ph, p, k, half).at[idx], landing(ph, p, m, half).at[idx], sem, to)

    def arrived(ph, p, name, idx=None):
        key = (ph, p, name) if idx is None else (ph, p, name, idx)
        if key in flights:
            flights.pop(key).wait_recv()
        _, m, _, half = plan[name]
        ref = landing(ph, p, m, half)
        return ref if idx is None else ref.at[idx]

    def add_into(ref, others):
        total = ref[...].astype(F32)
        for o in others:
            total = total + o[...].astype(F32)
        ref[...] = total.astype(BF)

    def onward(ph, p):
        for sign, idx in (("-", 0), ("+", 1), ("-", 1), ("+", 0)):
            got = arrived(ph, p, "a" + sign)
            _, _, k, half = plan["b" + sign]
            add_into(piece(ph, p, k, half).at[idx], [got.at[idx]])
            post_part(ph, p, "b" + sign, idx)

    def direct(p, k):
        return remote(own[p].at[0, 0, k], rx3[p].at[k - 1], 48 + p * 3 + k - 1, dev(axes[p][2], k))

    def settle(ph):
        for k in (2, 1, 3, 0):
            for p in (2, 0, 1):
                idx = k % 2
                if k < 2:
                    refs = [arrived(ph, p, "c-").at[idx], arrived(ph, p, "b+", idx)]
                else:
                    refs = [arrived(ph, p, "c+").at[idx], arrived(ph, p, "b-", idx)]
                add_into(own[p].at[(0,) * (ph + 1) + (k,)], refs)
                if ph:
                    if k:
                        last[p].append(direct(p, k))
                elif k == 2:
                    post(1, p, "a+"), post(1, p, "a-")
                elif k:
                    post(1, p, "c+" if k == 1 else "c-")

    last = ([], [], [])

    for k in range(4):
        blocks(2, k, 0, 2)
    for n in ("a+", "a-", "c+"):
        post(0, 2, n)
    blocks(0, 2, 0, 4)
    for j in range(4):
        quant_g(1, 1, j)
    post(0, 0, "a+"), post(0, 0, "a-")
    blocks(1, 2, 0, 4)
    for j in (2, 3):
        quant_g(1, 2, j)
    post(0, 1, "a+"), post(0, 1, "a-")
    for k in range(4):
        blocks(2, k, 2, 2)
    post(0, 2, "c-")
    for p in (0, 1):
        for k in (1, 3):
            blocks(p, k, 0, 4)
            post(0, p, "c+" if k == 1 else "c-")
    for p in (0, 1):
        blocks(p, 0, 0, 4)

    lax.fori_loop(3, 6, gh_step, 0)

    for p in (2, 0, 1):
        onward(0, p)
    lax.fori_loop(6, FFS // GH, gh_step, 0)
    settle(0)
    for p in (2, 0, 1):
        onward(1, p)
    settle(1)
    for p in (2, 0, 1):
        cols = slice(p * 128, p * 128 + 128)
        lo, size = EXTRA[p]
        for e in last[p]:
            e.wait_recv()
        total = own[p][0, 0, 0].astype(F32)
        for d in range(3):
            total = total + rx3[p][d].astype(F32)
        wg_ref[:, cols] = total[:ROWS]
        wg_ref[lo : lo + size, 384:512] = total[ROWS:]
    for s in sends[-SENDS:]:
        s.wait_send()


def finish(gh, wg, pk, gh_out, wg_out, ha_out, ga_out, wg_v, ha_v, ga_v, osem):
    outs = [pltpu.make_async_copy(gh, gh_out, osem.at[0])]
    outs[0].start()
    wg_v[...] = wg[...] * np.float32(1.0 / np.sqrt(SEQ * REPLICAS))
    outs.append(pltpu.make_async_copy(wg_v, wg_out, osem.at[1]))
    outs[1].start()
    ctx = lax.axis_index("ctx")
    ga_v[...] = pk[:, pl.ds(pl.multiple_of(FFS + ctx * 256, 256), 256)]
    outs.append(pltpu.make_async_copy(ga_v, ga_out, osem.at[2]))
    outs[2].start()
    some = pk[:, 0:ROWS]
    for k in range(1, 16):
        some = jnp.where(ctx == k, pk[:, k * ROWS : (k + 1) * ROWS], some)
    ha_v[...] = some
    outs.append(pltpu.make_async_copy(ha_v, ha_out, osem.at[3]))
    outs[3].start()
    for out in outs:
        out.wait()


def on_device(grad_out, hidden, down_weight):
    vm = pltpu.VMEM
    dma = pltpu.SemaphoreType.DMA
    heights = (144, 144, 160)
    scratch = [
        vm((TOK, D), BF), vm((TOK, FFS), BF), vm((TOK, D // 2), BF),
        vm((FFS, D), BF),
        vm((FFS, 2 * TOK), BF), vm((4, 2 * TOK, 512), BF), vm((2, 1, PEAKS), F32),
        vm((16, 384), F32), vm((16, 384), BF), vm((16, 384), BF), vm((16, 384), BF),
        vm((3, 16, 384), BF), vm((3, 16, 384), BF), vm((16, 384), BF),
    ]
    scratch += [vm((4, 4, 4, n, 128), BF) for n in heights]
    scratch += [vm((6, 2, 4, n, 128), BF) for n in heights]
    scratch += [vm((6, 2, n, 128), BF) for n in heights]
    scratch += [vm((3, n, 128), BF) for n in heights]
    scratch += [dma((5,)), dma((7,)), dma((SENDS,)), dma((76,))]
    hbm = pl.BlockSpec(memory_space=pltpu.HBM)
    vmspace = pl.BlockSpec(memory_space=pltpu.VMEM)
    gh, wg, peaks = pl.pallas_call(
        kernel,
        out_shape=(
            jax.ShapeDtypeStruct((TOK, FFS), BF),
            jax.ShapeDtypeStruct((ROWS, 512), F32),
            jax.ShapeDtypeStruct((1, PEAKS), F32),
        ),
        in_specs=[hbm] * 3,
        out_specs=(vmspace, vmspace, vmspace),
        scratch_shapes=scratch,
        compiler_params=pltpu.CompilerParams(
            collective_id=0, has_side_effects=True, vmem_limit_bytes=54_000_000),
    )(grad_out[0], hidden[0], down_weight)
    gh, wg, ha, ga = pl.pallas_call(
        finish,
        out_shape=(
            jax.ShapeDtypeStruct((TOK, FFS), BF),
            jax.ShapeDtypeStruct((ROWS, 512), F32),
            jax.ShapeDtypeStruct((1, ROWS), F32),
            jax.ShapeDtypeStruct((1, 256), F32),
        ),
        in_specs=[vmspace, vmspace, vmspace],
        out_specs=(hbm,) * 4,
        scratch_shapes=[vm((ROWS, 512), F32), vm((1, ROWS), F32), vm((1, 256), F32), dma((4,))],
        compiler_params=pltpu.CompilerParams(vmem_limit_bytes=8 * 1024 * 1024),
    )(gh, wg, peaks)
    return (gh[None], wg, ha, ga)


def solution(mesh):
    placed = (P("dp", "ctx", None), P("dp", "ctx", None), P())
    return jax.shard_map(
        on_device,
        mesh=mesh,
        in_specs=placed,
        out_specs=(P("dp", "ctx", None), P("ctx", "dp"), P("dp", "ctx"), P("dp", "ctx")),
        check_vma=False,
    )
```

```python
import functools

import jax
import jax.numpy as jnp
import numpy as np
from jax import lax
from jax.experimental import pallas as pl
from jax.experimental.pallas import tpu as pltpu
from jax.sharding import PartitionSpec as P

CEILING = 448.0
D, FFS, SEQ, REPLICAS = 4096, 1792, 6144, 8
TOK = 384
BF = jnp.bfloat16
F32 = jnp.float32
MESH = pl.DeviceIdType.MESH
NUDGE = np.float32(1 + 2.0**-21)
ROWS = 112
EXTRA = ((0, 32), (32, 32), (64, 48))
PEAKS = FFS + D
SENDS = 22
GH = 256


def kernel(g_hbm, h_hbm, w_hbm, gh_v, wg_ref, pk_out,
           g_own, h_own, g_peer, w_v, hqt, gq, pk,
           stage, am1, am2, am3, amy, amz, amp,
           own0, own1, own2, r10, r11, r12, r20, r21, r22, r30, r31, r32,
           lsem, wsem, ssem, rsem):
    ctx = lax.axis_index("ctx")
    dp = lax.axis_index("dp")
    z, y, x, c = ctx // 4, ctx % 4, dp // 2, dp % 2
    own, rx1, rx2, rx3 = (own0, own1, own2), (r10, r11, r12), (r20, r21, r22), (r30, r31, r32)

    def dev(axis, step):
        zz, yy, xx, cc = z, y, x, c
        if axis == "z":
            zz = (z + step) % 4
        elif axis == "y":
            yy = (y + step) % 4
        elif axis == "x":
            xx = (x + step) % 4
        else:
            cc = 1 - c
        return (zz * 4 + yy, xx * 2 + cc)

    lh = pltpu.make_async_copy(h_hbm, h_own, lsem.at[0])
    lh.start()
    lg = []
    for i in range(4):
        at = pl.ds(i * 1024, 1024)
        lg.append(pltpu.make_async_copy(g_hbm.at[:, at], g_own.at[:, at], lsem.at[1 + i]))
        lg[-1].start()

    def wcopy(j):
        at = pl.ds(pl.multiple_of(j * GH, GH), GH)
        return pltpu.make_async_copy(w_hbm.at[at, :], w_v.at[at, :], wsem.at[j])

    barrier = pltpu.get_barrier_semaphore()
    friends = [dev("y", d) for d in (1, 2, 3)] + [dev("z", d) for d in (1, 2, 3)]
    friends += [dev("x", d) for d in (1, 2, 3)] + [dev("c", 1)]
    for f in friends:
        pl.semaphore_signal(barrier, inc=1, device_id=f, device_id_type=MESH)

    sends = []

    def remote(src, dst, i, to, base=0):
        slot = len(sends) % SENDS
        if len(sends) >= SENDS:
            sends[-SENDS].wait_send()
        copy = pltpu.make_async_remote_copy(
            src_ref=src, dst_ref=dst, send_sem=ssem.at[slot], recv_sem=rsem.at[base + i],
            device_id=to, device_id_type=MESH)
        copy.start()
        sends.append(copy)
        return copy

    small = 56

    def peak_row(ref, lo, size):
        at = pl.ds(pl.multiple_of(lo, 128), size)
        return jnp.max(jnp.abs(ref[:, at].astype(F32)), axis=0, keepdims=True)

    stage[...] = jnp.zeros_like(stage)
    lh.wait()

    def h_peaks(i, _):
        at = pl.multiple_of(i * 256, 256)
        pk[0, :, pl.ds(at, 256)] = peak_row(h_own, at, 256)
        return 0

    lax.fori_loop(0, FFS // 256, h_peaks, 0)
    pl.semaphore_wait(barrier, len(friends))
    peer = dev("c", 1)
    wcopy(0).start()
    swaps = []
    for i in range(4):
        lg[i].wait()
        src = pl.ds(pl.multiple_of(i * 1024 + (1 - c) * 512, 512), 512)
        swaps.append(remote(g_own.at[:, src], g_peer.at[:, pl.ds(i * 512, 512)], 1 + i, peer, small))

        def g_peaks(k, _, i=i):
            at = pl.multiple_of(i * 1024 + k * 256, 256)
            pk[0, :, pl.ds(FFS + at, 256)] = peak_row(g_own, at, 256)
            return 0

        lax.fori_loop(0, 4, g_peaks, 0)

    def spread(n):
        for r in range(16):
            size = 384 if r < 15 else 128
            yield r, slice(0, size), slice(r * 384, r * 384 + size)

    for j in range(1, FFS // GH):
        wcopy(j).start()
    for r, a, b in spread(16):
        stage[r : r + 1, a] = pk[0, :, b]
    am1[...] = stage[...].astype(BF)
    gets = [remote(am1, amy.at[d - 1], 5 + d - 1, dev("y", d), small) for d in (2, 1, 3)]

    def gh_step(j, _):
        wcopy(j).wait()
        at = pl.ds(pl.multiple_of(j * GH, GH), GH)
        res = lax.dot_general(
            g_own[...], w_v[at, :], (((1,), (1,)), ((), ())), preferred_element_type=F32)
        gh_v[:, at] = res.astype(BF)
        return 0

    gh_step(0, 0)
    for e in gets:
        e.wait_recv()
    am2[...] = jnp.maximum(
        jnp.maximum(am1[...].astype(F32), amy[0].astype(F32)),
        jnp.maximum(amy[1].astype(F32), amy[2].astype(F32))).astype(BF)
    gets = [remote(am2, amz.at[d - 1], 8 + d - 1, dev("z", d), small) for d in (2, 1, 3)]
    lax.fori_loop(1, 3, gh_step, 0)
    for e in gets:
        e.wait_recv()
    top = jnp.maximum(
        jnp.maximum(am2[...].astype(F32), amz[0].astype(F32)),
        jnp.maximum(amz[1].astype(F32), amz[2].astype(F32)))
    am3[...] = top.astype(BF)
    swap_peaks = remote(am3, amp, 11, peer, small)

    def unpack(r, values):
        stage[...] = jnp.maximum(values, 1.0)
        for k, a, b in spread(16):
            pk[r, :, b] = stage[k : k + 1, a]

    unpack(0, top)
    pk_out[...] = pk[0]

    def on_grid(values, peaks):
        v = values.astype(F32) * ((CEILING / peaks) * 1024.0)
        u = v.astype(jnp.int32).astype(F32) * NUDGE
        big = jnp.maximum(jnp.abs(u) * 2.0**20, 1.5 * 2.0**24)
        return (((u + big) - big) * (peaks / CEILING * 2.0**-10)).astype(BF)

    def quant_g(r, q, j, lo=0, rows=TOK):
        xx = (x + (6 - j) % 4) % 4
        home = xx * 1024 + c * 512 + q * 128
        at = pl.ds(pl.multiple_of(home if r == 0 else xx * 512 + q * 128, 128), 128)
        peaks = pk[r, :, pl.ds(pl.multiple_of(FFS + home, 128), 128)]
        ref = g_own if r == 0 else g_peer
        to = pl.ds(pl.multiple_of(j * 128, 128), 128)
        gq[q, pl.ds(r * TOK + lo, rows), to] = on_grid(ref[pl.ds(lo, rows), at], peaks)

    hsends = []
    for i in range(FFS // 256):
        at = pl.ds(i * 256, 256)
        hqt[at, 0:TOK] = on_grid(h_own[:, at], pk[0, :, at]).T
        if i in (2, 4, 6):
            prev = pl.ds((i - 2) * 256, 512)
            hsends.append(remote(hqt.at[prev, 0:TOK], hqt.at[prev, TOK:], i // 2 - 1, peer, 68))
    for j in range(2):
        for q in (2, 3):
            quant_g(0, q, j)
        if j == 0:
            prev = pl.ds(FFS - 256, 256)
            hsends.append(remote(hqt.at[prev, 0:TOK], hqt.at[prev, TOK:], 3, peer, 68))
    for j in range(4):
        quant_g(0, 0, j)
        quant_g(0, 1, j)
        if j > 1:
            quant_g(0, 2, j), quant_g(0, 3, j)
    swap_peaks.wait_recv()
    unpack(1, amp[...].astype(F32))
    for e in swaps:
        e.wait_recv()
    for j in range(2):
        for q in (2, 3):
            quant_g(1, q, j)
    for j in range(4):
        quant_g(1, 0, j)
        if j > 1:
            quant_g(1, 3, j)
    for e in hsends:
        e.wait_recv()

    def product(q, offsets, size, cols):
        left = jnp.concatenate(
            [hqt[pl.ds(pl.multiple_of(o, 16), size), :] for o in offsets], axis=0)
        return jnp.dot(left, gq[q, :, cols], preferred_element_type=F32).astype(BF)

    def blocks(p, k, j0, count):
        if p == 1:
            base = [o * 448 + ((y + k) % 4) * ROWS for o in range(4)]
        else:
            base = [((z + k) % 4) * 448 + o * ROWS for o in range(4)]
        lo, size = EXTRA[p]
        cols = slice(j0 * 128, (j0 + count) * 128)
        main = product(p, base, ROWS, cols)
        more = product(3, [b + lo for b in base], size, cols)
        for o in range(4):
            away = (o - z) % 4 if p == 1 else (o - y) % 4
            for j in range(count):
                xr = (6 - j0 - j) % 4
                if p == 0:
                    to = own0.at[k, away, xr]
                elif p == 1:
                    to = own1.at[k, xr, away]
                else:
                    to = own2.at[xr, k, away]
                at = slice(j * 128, j * 128 + 128)
                to[0:ROWS, :] = main[o * ROWS : (o + 1) * ROWS, at]
                to[ROWS : ROWS + size, :] = more[o * size : (o + 1) * size, at]

    axes = (("z", "y", "x"), ("y", "x", "z"), ("x", "z", "y"))

    def piece(ph, p, k, half):
        ref = own[p].at[k] if ph == 0 else own[p].at[0, k]
        return ref.at[pl.ds(2 * half, 2)]

    def landing(ph, p, m, half):
        return (rx1, rx2)[ph][p].at[m]

    flights = {}
    plan = {
        "a+": (0, 0, 2, 0), "c+": (0, 1, 1, 1), "b+": (0, 2, 1, 0),
        "a-": (1, 3, 2, 1), "c-": (1, 4, 3, 0), "b-": (1, 5, 3, 1),
    }

    def post(ph, p, name):
        way, m, k, half = plan[name]
        to = dev(axes[p][ph], 1 if way == 0 else 3)
        flights[ph, p, name] = remote(
            piece(ph, p, k, half), landing(ph, p, m, half), (ph * 3 + p) * 8 + m, to)

    def post_part(ph, p, name, idx):
        way, m, k, half = plan[name]
        to = dev(axes[p][ph], 1 if way == 0 else 3)
        sem = (ph * 3 + p) * 8 + (m if idx == 0 else 6 + way)
        flights[ph, p, name, idx] = remote(
            piece(ph, p, k, half).at[idx], landing(ph, p, m, half).at[idx], sem, to)

    def arrived(ph, p, name, idx=None):
        key = (ph, p, name) if idx is None else (ph, p, name, idx)
        if key in flights:
            flights.pop(key).wait_recv()
        _, m, _, half = plan[name]
        ref = landing(ph, p, m, half)
        return ref if idx is None else ref.at[idx]

    def add_into(ref, others):
        total = ref[...].astype(F32)
        for o in others:
            total = total + o[...].astype(F32)
        ref[...] = total.astype(BF)

    def onward(ph, p):
        for sign, idx in (("-", 0), ("+", 1), ("-", 1), ("+", 0)):
            got = arrived(ph, p, "a" + sign)
            _, _, k, half = plan["b" + sign]
            add_into(piece(ph, p, k, half).at[idx], [got.at[idx]])
            post_part(ph, p, "b" + sign, idx)

    def direct(p, k):
        return remote(own[p].at[0, 0, k], rx3[p].at[k - 1], 48 + p * 3 + k - 1, dev(axes[p][2], k))

    def settle(ph):
        for k in (2, 1, 3, 0):
            for p in (2, 0, 1):
                idx = k % 2
                if k < 2:
                    refs = [arrived(ph, p, "c-").at[idx], arrived(ph, p, "b+", idx)]
                else:
                    refs = [arrived(ph, p, "c+").at[idx], arrived(ph, p, "b-", idx)]
                add_into(own[p].at[(0,) * (ph + 1) + (k,)], refs)
                if ph:
                    if k:
                        last[p].append(direct(p, k))
                elif k == 2:
                    post(1, p, "a+"), post(1, p, "a-")
                elif k:
                    post(1, p, "c+" if k == 1 else "c-")

    last = ([], [], [])

    for k in range(4):
        blocks(2, k, 0, 2)
    for n in ("a+", "a-", "c+"):
        post(0, 2, n)
    blocks(0, 2, 0, 4)
    for j in range(4):
        quant_g(1, 1, j)
    post(0, 0, "a+"), post(0, 0, "a-")
    blocks(1, 2, 0, 4)
    for j in (2, 3):
        quant_g(1, 2, j)
    post(0, 1, "a+"), post(0, 1, "a-")
    for k in range(4):
        blocks(2, k, 2, 2)
    post(0, 2, "c-")
    for p in (0, 1):
        for k in (1, 3):
            blocks(p, k, 0, 4)
            post(0, p, "c+" if k == 1 else "c-")
    for p in (0, 1):
        blocks(p, 0, 0, 4)

    lax.fori_loop(3, 6, gh_step, 0)

    for p in (2, 0, 1):
        onward(0, p)
    lax.fori_loop(6, FFS // GH, gh_step, 0)
    settle(0)
    for p in (2, 0, 1):
        onward(1, p)
    settle(1)
    for p in (2, 0, 1):
        cols = slice(p * 128, p * 128 + 128)
        lo, size = EXTRA[p]
        for e in last[p]:
            e.wait_recv()
        total = own[p][0, 0, 0].astype(F32)
        for d in range(3):
            total = total + rx3[p][d].astype(F32)
        wg_ref[:, cols] = total[:ROWS]
        wg_ref[lo : lo + size, 384:512] = total[ROWS:]
    for s in sends[-SENDS:]:
        s.wait_send()


def finish(gh, wg, pk, gh_out, wg_out, ha_out, ga_out, wg_v, ha_v, ga_v, osem):
    outs = [pltpu.make_async_copy(gh, gh_out, osem.at[0])]
    outs[0].start()
    wg_v[...] = wg[...] * np.float32(1.0 / np.sqrt(SEQ * REPLICAS))
    outs.append(pltpu.make_async_copy(wg_v, wg_out, osem.at[1]))
    outs[1].start()
    ctx = lax.axis_index("ctx")
    ga_v[...] = pk[:, pl.ds(pl.multiple_of(FFS + ctx * 256, 256), 256)]
    outs.append(pltpu.make_async_copy(ga_v, ga_out, osem.at[2]))
    outs[2].start()
    some = pk[:, 0:ROWS]
    for k in range(1, 16):
        some = jnp.where(ctx == k, pk[:, k * ROWS : (k + 1) * ROWS], some)
    ha_v[...] = some
    outs.append(pltpu.make_async_copy(ha_v, ha_out, osem.at[3]))
    outs[3].start()
    for out in outs:
        out.wait()


def on_device(grad_out, hidden, down_weight):
    vm = pltpu.VMEM
    dma = pltpu.SemaphoreType.DMA
    heights = (144, 144, 160)
    scratch = [
        vm((TOK, D), BF), vm((TOK, FFS), BF), vm((TOK, D // 2), BF),
        vm((FFS, D), BF),
        vm((FFS, 2 * TOK), BF), vm((4, 2 * TOK, 512), BF), vm((2, 1, PEAKS), F32),
        vm((16, 384), F32), vm((16, 384), BF), vm((16, 384), BF), vm((16, 384), BF),
        vm((3, 16, 384), BF), vm((3, 16, 384), BF), vm((16, 384), BF),
    ]
    scratch += [vm((4, 4, 4, n, 128), BF) for n in heights]
    scratch += [vm((6, 2, 4, n, 128), BF) for n in heights]
    scratch += [vm((6, 2, n, 128), BF) for n in heights]
    scratch += [vm((3, n, 128), BF) for n in heights]
    scratch += [dma((5,)), dma((7,)), dma((SENDS,)), dma((72,))]
    hbm = pl.BlockSpec(memory_space=pltpu.HBM)
    vmspace = pl.BlockSpec(memory_space=pltpu.VMEM)
    gh, wg, peaks = pl.pallas_call(
        kernel,
        out_shape=(
            jax.ShapeDtypeStruct((TOK, FFS), BF),
            jax.ShapeDtypeStruct((ROWS, 512), F32),
            jax.ShapeDtypeStruct((1, PEAKS), F32),
        ),
        in_specs=[hbm] * 3,
        out_specs=(vmspace, vmspace, vmspace),
        scratch_shapes=scratch,
        compiler_params=pltpu.CompilerParams(
            collective_id=0, has_side_effects=True, vmem_limit_bytes=54_000_000),
    )(grad_out[0], hidden[0], down_weight)
    gh, wg, ha, ga = pl.pallas_call(
        finish,
        out_shape=(
            jax.ShapeDtypeStruct((TOK, FFS), BF),
            jax.ShapeDtypeStruct((ROWS, 512), F32),
            jax.ShapeDtypeStruct((1, ROWS), F32),
            jax.ShapeDtypeStruct((1, 256), F32),
        ),
        in_specs=[vmspace, vmspace, vmspace],
        out_specs=(hbm,) * 4,
        scratch_shapes=[vm((ROWS, 512), F32), vm((1, ROWS), F32), vm((1, 256), F32), dma((4,))],
        compiler_params=pltpu.CompilerParams(vmem_limit_bytes=8 * 1024 * 1024),
    )(gh, wg, peaks)
    return (gh[None], wg, ha, ga)


def solution(mesh):
    placed = (P("dp", "ctx", None), P("dp", "ctx", None), P())
    return jax.shard_map(
        on_device,
        mesh=mesh,
        in_specs=placed,
        out_specs=(P("dp", "ctx", None), P("ctx", "dp"), P("dp", "ctx"), P("dp", "ctx")),
        check_vma=False,
    )
```
